256 devices in a mesh: band: 8 (over y, core), ga: 32 (over z, x).
Axes of the slice: x: 4, y: 4, z: 8, core: 2. Of those that a mesh axis runs over, the one named last changes fastest.
Arguments:
- density: float32 [160, 160, 160], P('ga'), may hold values from -6 to 6
- stick_column: int32 [20480], replicated, may hold values from 0 to 25599, as said below
- vloc: float32 [2, 160, 20480], P(None, None, 'ga'), may hold values from -0.0034179688 to 0.0034179688
- positions: float32 [3, 32], replicated, may hold values from 0 to 1
- species: int32 [32], replicated, may hold values from 0 to 1
- psi: bfloat16 [270336, 2, 1024], P('ga', None, 'band'), may hold values from -6 to 6
- miller_wave: int32 [3, 270336], P(None, 'ga'), may hold values from -40 to 40
- proj_radial: float32 [2, 8, 270336], P(None, None, 'ga'), may hold values from -0.01171875 to 0.01171875
- proj_count: int32 [2], replicated, may hold values from 4 to 8
- dcoef: float32 [2, 8, 8], replicated, may hold values from -0.0625 to 0.0625
- occupation: float32 [1024], P('band'), may hold values from 0 to 2
Outputs:
- density_sticks: float32 [2, 160, 20480], P(None, None, 'ga')
- forces: float32 [3, 32], replicated
The draws below stay inside these ranges and needn't reach their ends.
Inputs may be any that keep to these rules, and one draw needn't show every extreme that they name: `stick_column`: distinct columns of the 160 by 160 frequency plane.
All inputs are finite; a program needn't handle non-finite values.
Results may differ from the reference program's by a relative error of at most 0.0036.
Values sent between devices are 32-bit elements; how exact they have to be, the bound alone decides.
No kernel may reach another device: no remote copies, remote signals or barrier semaphores. Data moves between devices by JAX's collectives and lax.ppermute only.
A program may use at most 128 MiB of HBM per device.

```python
import math
import jax
import jax.numpy as jnp
from jax import lax

NX = 160
NY = 160
NZ = 160
NSTICK = 20480
NPW = 270336
BANDS = 1024
NSP = 2
PSLOT = 8
ATOMS = 32


def draw_stick_column(key, part):
    return jax.random.permutation(key, NX * NY)[:NSTICK].astype(jnp.int32)


def touch_ends(drawn, rng, low, largest):
    dims = drawn.shape
    index_at = [jax.random.randint(jax.random.fold_in(rng, axis), (), 0, dims[axis]) for axis in range(len(dims))]
    drawn = drawn.at[tuple(index_at)].set(low)
    longest = dims.index(max(dims))
    index_at[longest] = (index_at[longest] + 1) % dims[longest]
    return drawn.at[tuple(index_at)].set(largest)


def levels(rng, extent, cuts, smallest, largest):
    def one(axis_at, blocks):
        heights = jax.random.uniform(jax.random.fold_in(jax.random.fold_in(rng, 6), axis_at), (blocks,), jnp.float32, smallest / len(cuts), largest / len(cuts))
        return jnp.repeat(jnp.exp(heights), extent[axis_at] // blocks).reshape((-1,) + (1,) * (len(extent) - axis_at - 1))

    factor_of = one(*cuts[0])
    for cut in cuts[1:]:
        factor_of = factor_of * one(*cut)
    return factor_of


def gaussian(stream_key, shape, deviation, reach, cuts=(), kind=jnp.bfloat16):
    array = deviation * jax.random.normal(stream_key, shape, jnp.float32)
    if cuts:
        array = array * levels(stream_key, shape, cuts, -0.22, 0.18)
    return jnp.clip(array, -reach, reach).astype(kind)


def setup_inputs(seed: int = 0) -> dict:
    streams_of = jax.random.split(jax.random.key(seed), 12)
    density = gaussian(streams_of[0], (NZ, NX, NY), 1.0, 6.0, ((0, 32),), jnp.float32)
    stick_column = draw_stick_column(jax.random.fold_in(streams_of[11], 71), 0)
    vloc = gaussian(streams_of[2], (NSP, NZ, NSTICK), (NZ * NSTICK) ** -0.5, 0.0034179688, ((2, 32),), jnp.float32)
    positions = jnp.clip(jax.random.uniform(streams_of[3], (3, ATOMS), jnp.float32, 0.0, 1.0), 0.0, 1.0)
    species = touch_ends(jax.random.randint(streams_of[4], (ATOMS,), 0, NSP), jax.random.fold_in(streams_of[4], 1), 0, NSP - 1).astype(jnp.int32)
    psi = gaussian(streams_of[5], (NPW, 2, BANDS), 1.0, 6.0, ((0, 32), (2, 8)))
    miller_wave = touch_ends(jax.random.randint(streams_of[6], (3, NPW), 0 - NX // 4, NX // 4 + 1), jax.random.fold_in(streams_of[6], 1), 0 - NX // 4, (NX // 4 + 1) - 1).astype(jnp.int32)
    proj_radial = gaussian(streams_of[7], (NSP, PSLOT, NPW), NPW ** -0.5, 0.01171875, ((2, 32),), jnp.float32)
    proj_count = jax.random.randint(streams_of[8], (NSP,), 4, PSLOT + 1).astype(jnp.int32)
    dcoef = gaussian(streams_of[9], (NSP, PSLOT, PSLOT), 0.004, 0.0625, (), jnp.float32)
    occupation = jnp.clip(2.0 * jax.random.uniform(streams_of[10], (BANDS,), jnp.float32) ** levels(streams_of[10], (BANDS,), ((0, 8),), -0.2, 0.2), 0.0, 2.0)
    return dict(density=density, stick_column=stick_column, vloc=vloc, positions=positions, species=species, psi=psi, miller_wave=miller_wave, proj_radial=proj_radial, proj_count=proj_count, dcoef=dcoef, occupation=occupation)


TWO_PI = 2.0 * math.pi
EXACT = lax.Precision.HIGHEST

def frequency(index, count):
    return jnp.where(index >= count // 2, index - count, index)

def reference(density, stick_column, vloc, positions, species, psi, miller_wave, proj_radial, proj_count, dcoef, occupation):
    spectrum = jnp.fft.fftn(density) * (1.0 / math.sqrt(NX * NY * NZ))
    picked = spectrum.reshape(NZ, NX * NY)[:, stick_column]
    stick_re = jnp.real(picked)
    stick_im = jnp.imag(picked)
    density_sticks = jnp.stack([stick_re, stick_im])
    freq_x = frequency(stick_column // NY, NX).astype(jnp.float32)
    freq_y = frequency(stick_column % NY, NY).astype(jnp.float32)
    freq_z = frequency(jnp.arange(NZ, dtype=jnp.int32), NZ).astype(jnp.float32)
    wave_x = TWO_PI / NX * freq_x
    wave_y = TWO_PI / NY * freq_y
    wave_z = TWO_PI / NZ * freq_z

    def local_atom(atom):
        place = positions[:, atom]
        angle = TWO_PI * (freq_z[:, None] * place[2] + (freq_x * place[0] + freq_y * place[1])[None, :])
        weight = vloc[species[atom]] * (stick_re * jnp.sin(angle) + stick_im * jnp.cos(angle))
        return jnp.stack([jnp.sum(weight * wave_x[None, :]), jnp.sum(weight * wave_y[None, :]), jnp.sum(weight * wave_z[:, None])])
    local_force = lax.map(local_atom, jnp.arange(ATOMS, dtype=jnp.int32)).T
    miller_f = miller_wave.astype(jnp.float32)
    weights = jnp.stack([jnp.ones_like(miller_f[0]), TWO_PI / NX * miller_f[0], TWO_PI / NY * miller_f[1], TWO_PI / NZ * miller_f[2]])
    psi_flat = psi.reshape(NPW, 2 * BANDS)
    live_slots = (jnp.arange(PSLOT, dtype=jnp.int32)[None, :] < proj_count[:, None]).astype(jnp.float32)

    def nonlocal_atom(atom):
        place = positions[:, atom]
        kind = species[atom]
        phase = TWO_PI * (place[0] * miller_f[0] + place[1] * miller_f[1] + place[2] * miller_f[2])
        radial = proj_radial[kind]
        parts = jnp.stack([radial * jnp.cos(phase)[None, :], radial * jnp.sin(phase)[None, :]], axis=1)
        table = (parts[:, None] * weights[None, :, None, :]).astype(jnp.bfloat16)
        product = jnp.dot(table.reshape(PSLOT * 8, NPW), psi_flat, preferred_element_type=jnp.float32)
        product = product.reshape(PSLOT, 4, 2, 2, BANDS)
        proj_re = product[:, :, 0, 0] - product[:, :, 1, 1]
        proj_im = product[:, :, 0, 1] + product[:, :, 1, 0]
        live = live_slots[kind]
        coupling = dcoef[kind] * live[:, None] * live[None, :]
        mixed_re = jnp.einsum('ij,jcn->icn', coupling, proj_re[:, 1:], precision=EXACT)
        mixed_im = jnp.einsum('ij,jcn->icn', coupling, proj_im[:, 1:], precision=EXACT)
        value = proj_re[:, 0][:, None, :] * mixed_im - proj_im[:, 0][:, None, :] * mixed_re
        return 2.0 * jnp.einsum('icn,n->c', value, occupation, precision=EXACT)
    nonlocal_force = lax.map(nonlocal_atom, jnp.arange(ATOMS, dtype=jnp.int32)).T
    forces = local_force + nonlocal_force
    return (density_sticks, forces)
```

```python
import math

import jax
import jax.numpy as jnp
import numpy as np
from jax import lax
from jax.experimental import pallas as pl
from jax.experimental.pallas import tpu as pltpu
from jax.sharding import Mesh
from jax.sharding import PartitionSpec as P


N = 160
HALF = 81
ATOMS = 32
SLOTS = 8
GA = ("ga_0", "ga_1")
BAND = ("band_0", "band_1")
BAND_GA = ("band_0", "band_1", "ga_0", "ga_1")
GA_COUNT = 32
BAND_COUNT = 8
PLANES = 5
OWN = 640
PART = OWN // BAND_COUNT
STICKS = GA_COUNT * PART
ROWS_E = 88
ROWS_O = 80
ROWS = ROWS_E + ROWS_O
CHUNK = 256
WAVES = 8448
STEP = 768
TWO_PI = 2.0 * math.pi
NORM = 1.0 / math.sqrt(N * N * N)
F32 = jnp.float32
BF16 = jnp.bfloat16

COS_POLY = (
    6.528658390045166,
    -25.967599868774414,
    60.16762924194336,
    -85.45014190673828,
    64.93911743164062,
    -19.73920440673828,
    1.0,
)
SIN_POLY = (
    3.2381374835968018,
    -14.899847030639648,
    42.02592849731445,
    -76.70301818847656,
    81.60513305664062,
    -41.34170150756836,
    6.2831854820251465,
)


def split_np(table, pieces):
    out = []
    rest = np.asarray(table, np.float64)
    for _ in range(pieces):
        part = np.asarray(rest, np.float32).astype(BF16)
        out.append(part)
        rest = rest - part.astype(np.float64)
    return out


def angles(a, b):
    return TWO_PI / N * ((np.asarray(a)[:, None] * np.asarray(b)[None, :]) % N)


def fold_table():
    fold = np.zeros((ROWS, N), np.float32)
    for x in range(HALF):
        fold[x, x] = 1.0
        fold[x, (N - x) % N] = 1.0
    for x in range(1, N // 2):
        fold[ROWS_E + x - 1, x] = 1.0
        fold[ROWS_E + x - 1, N - x] = -1.0
    return fold.astype(BF16)


def plane_tables():
    freq = np.arange(HALF)
    cos_y = np.zeros((N, 256))
    sin_y = np.zeros((N, 256))
    for third in range(3):
        cos_y[:, third * HALF : (third + 1) * HALF] = np.cos(angles(np.arange(N), freq))
        sin_y[:, third * HALF : (third + 1) * HALF] = np.sin(angles(np.arange(N), freq))
    cos_hi, cos_lo = split_np(cos_y, 2)
    sin_hi, sin_lo = split_np(sin_y, 2)
    y_table = np.stack([cos_hi, cos_lo, sin_hi, sin_lo])
    cos_x = split_np(np.cos(angles(np.arange(HALF), freq)), 3)
    sin_x = split_np(np.sin(angles(np.arange(1, N // 2), freq)), 3)
    x_table = np.zeros((ROWS, 256), BF16)
    for third in range(3):
        x_table[:HALF, third * HALF : (third + 1) * HALF] = cos_x[third]
        x_table[ROWS_E : ROWS_E + N // 2 - 1, third * HALF : (third + 1) * HALF] = sin_x[third]
    return y_table, x_table


def depth_tables():
    angle = angles(np.arange(N), np.arange(N))
    table = np.zeros((2 * N, GA_COUNT * 8))
    for s in range(GA_COUNT):
        for p in range(PLANES):
            table[:N, 8 * s + p] = np.cos(angle[:, PLANES * s + p])
            table[N:, 8 * s + p] = np.sin(angle[:, PLANES * s + p])
    return np.stack(split_np(table, 2))


def parts_table():
    table = np.zeros((256, 256), np.float32)
    for g in range(128):
        table[g, 2 * g] = 1.0
        table[128 + g, 2 * g + 1] = 1.0
    return table.astype(BF16)


def dot(a, b):
    return jnp.dot(a, b, preferred_element_type=F32)


def halves(value):
    high = value.astype(BF16)
    return high, (value - high.astype(F32)).astype(BF16)


def thirds(value):
    high = value.astype(BF16)
    rest = value - high.astype(F32)
    mid = rest.astype(BF16)
    return high, mid, (rest - mid.astype(F32)).astype(BF16)


def dot_fine(a, b):
    a_high, a_low = halves(a)
    b_high, b_low = halves(b)
    return dot(a_high, b_high) + dot(a_high, b_low) + dot(a_low, b_high)


def cos_sin(turns):
    t = turns - jnp.round(turns)
    s = t * t
    cos = jnp.full_like(s, COS_POLY[0])
    for c in COS_POLY[1:]:
        cos = cos * s + c
    sin = jnp.full_like(s, SIN_POLY[0])
    for c in SIN_POLY[1:]:
        sin = sin * s + c
    return cos, sin * t


def frequency(index):
    return jnp.where(index >= N // 2, index - N, index)


def sticks_kernel(density_ref, column_ref, fold_ref, y_ref, x_ref, out_ref, left_ref, sums_ref):
    fold = fold_ref[...]
    folded = []
    for p in range(PLANES):
        high, mid, low = thirds(density_ref[p])
        folded.append(dot(fold, high) + dot(fold, mid) + dot(fold, low))
    folded = jnp.concatenate(folded, axis=0)
    e_high, e_low = halves(folded)
    lane = lax.broadcasted_iota(jnp.int32, (PLANES * ROWS, 256), 1)
    for part in range(2):
        spec = (
            dot(e_high, y_ref[2 * part])
            + dot(e_high, y_ref[2 * part + 1])
            + dot(e_low, y_ref[2 * part])
        )
        high = spec.astype(BF16).astype(F32)
        rest = spec - high
        mid = rest.astype(BF16).astype(F32)
        left = jnp.where(lane < HALF, high, jnp.where(lane < 2 * HALF, mid, rest - mid))
        left_ref[part] = left.astype(BF16)
    row = lax.broadcasted_iota(jnp.int32, (256, CHUNK), 0)
    row = jnp.where(
        row < HALF,
        row,
        jnp.where(row < 2 * HALF, row - HALF, jnp.where(row < 3 * HALF, row - 2 * HALF, -1)),
    )
    for chunk in range(STICKS // CHUNK):
        lanes = pl.ds(chunk * CHUNK, CHUNK)
        column = column_ref[0:1, lanes]
        column_x = lax.div(column, N)
        freq_x = frequency(column_x)
        freq_y = frequency(column - N * column_x)
        hit_x = row == jnp.abs(freq_x)
        hit_y = row == jnp.abs(freq_y)
        sign_x = jnp.where(freq_x < 0, -1.0, 1.0)
        sign_y = jnp.where(freq_y < 0, -1.0, 1.0)
        pick_cx = jnp.where(hit_x, 1.0, 0.0).astype(BF16)
        pick_sx = jnp.where(hit_x, sign_x, 0.0).astype(BF16)
        pick_cy = jnp.where(hit_y, 1.0, 0.0).astype(BF16)
        pick_sy = jnp.where(hit_y, sign_y, 0.0).astype(BF16)
        cos_x = dot(x_ref[0:ROWS_E], pick_cx)
        sin_x = dot(x_ref[ROWS_E:ROWS], pick_sx)
        t_cos = dot(left_ref[0], pick_cy)
        t_sin = dot(left_ref[1], pick_sy)
        real = []
        imag = []
        for p in range(PLANES):
            at = p * ROWS
            mid = at + ROWS_E
            end = at + ROWS
            re = (t_cos[at:mid] * cos_x).reshape(ROWS_E // 8, 8, CHUNK).sum(0) - (
                t_sin[mid:end] * sin_x
            ).reshape(ROWS_O // 8, 8, CHUNK).sum(0)
            im = (t_sin[at:mid] * cos_x).reshape(ROWS_E // 8, 8, CHUNK).sum(0) + (
                t_cos[mid:end] * sin_x
            ).reshape(ROWS_O // 8, 8, CHUNK).sum(0)
            real.append(re.sum(0, keepdims=True))
            imag.append(-im.sum(0, keepdims=True))
        blank = [jnp.zeros((1, CHUNK), F32)] * (8 - PLANES)
        sums_ref[0, :, lanes] = jnp.concatenate(real + blank, axis=0)
        sums_ref[1, :, lanes] = jnp.concatenate(imag + blank, axis=0)
    sums_ref[0, :, pl.ds(STICKS, 128)] = jnp.zeros((8, 128), F32)
    sums_ref[1, :, pl.ds(STICKS, 128)] = jnp.zeros((8, 128), F32)
    keep = lax.broadcasted_iota(jnp.int32, (8, 128), 1) < PART
    for d in range(GA_COUNT):
        first = d * PART // 128 * 128
        for part in range(2):
            window = sums_ref[part, :, pl.ds(first, 256)]
            shift = d * PART - first
            if shift:
                window = pltpu.roll(window, 256 - shift, 1)
            out_ref[d, :, pl.ds(128 * part, 128)] = jnp.where(keep, window[:, :128], 0.0)


def picked_radial(radial_ref, slot, kind):
    return jnp.where(kind, radial_ref[1, slot : slot + 1, :], radial_ref[0, slot : slot + 1, :])


def wave_turns(place_ref, miller):
    return (
        place_ref[:, 0:1] * miller[0:1]
        + place_ref[:, 1:2] * miller[1:2]
        + place_ref[:, 2:3] * miller[2:3]
    )


def project_kernel(
    psi_ref, miller_ref, radial_ref, place_ref, kind_ref, parts_ref, sticks_ref, out_ref, psi_out_ref, acc_ref
):
    step = pl.program_id(0)
    parts = parts_ref[...]
    pieces = []
    for k in range(STEP // 128):
        piece = dot(parts, psi_ref[pl.ds(256 * k, 256), :]).astype(BF16)
        pieces.append(jnp.concatenate([piece[:128], piece[128:]], axis=1))
    waves = jnp.concatenate(pieces, axis=0)
    psi_out_ref[...] = waves
    miller = miller_ref[...].astype(F32)
    cos, sin = cos_sin(wave_turns(place_ref, miller))
    kind = kind_ref[:, 0:1] == 1
    rows_cos = []
    rows_sin = []
    for slot in range(SLOTS):
        radial = picked_radial(radial_ref, slot, kind)
        rows_cos.append((radial * cos).astype(BF16))
        rows_sin.append((radial * sin).astype(BF16))
    product = dot(jnp.concatenate(rows_cos + rows_sin, axis=0), waves)

    @pl.when(step == 0)
    def _():
        acc_ref[...] = product

    @pl.when(step > 0)
    def _():
        acc_ref[...] += product

    @pl.when(step == pl.num_programs(0) - 1)
    def _():
        rows = ATOMS * SLOTS
        real = acc_ref[0:rows, 0:128] - acc_ref[rows : 2 * rows, 128:256]
        imag = acc_ref[0:rows, 128:256] + acc_ref[rows : 2 * rows, 0:128]
        out_ref[:, 0:8, :] = jnp.concatenate([real, imag], axis=1).reshape(GA_COUNT, 8, 256)
        out_ref[:, 8:16, :] = sticks_ref[...]


def depth_kernel(
    arrived_ref, table_ref, vloc_ref, place_ref, kind_ref, column_ref, own_ref, force_ref
):
    planes = arrived_ref[...].reshape(GA_COUNT * 8, 256)
    high, low = halves(planes)
    product = dot(table_ref[0], high) + dot(table_ref[0], low) + dot(table_ref[1], high)
    real = (product[:N, :128] + product[N:, 128:]) * NORM
    imag = (product[:N, 128:] - product[N:, :128]) * NORM
    own_ref[0] = real
    own_ref[1] = imag
    kind = kind_ref[:, 0:1] == 1
    column = column_ref[...]
    column_x = lax.div(column, N)
    freq_x = frequency(column_x).astype(F32)
    freq_y = frequency(column - N * column_x).astype(F32)
    freq_z = frequency(lax.broadcasted_iota(jnp.int32, (1, N), 1)).astype(F32)
    cos_z, sin_z = cos_sin(place_ref[:, 2:3] * freq_z)
    wave_z = TWO_PI / N * freq_z
    left = jnp.concatenate([cos_z, sin_z, cos_z * wave_z, sin_z * wave_z], axis=0)
    fields = []
    for s in range(2):
        fields.append(vloc_ref[s] * real)
        fields.append(vloc_ref[s] * imag)
    summed = dot_fine(left, jnp.concatenate(fields, axis=1))
    summed = jnp.where(
        jnp.concatenate([kind] * 4, axis=0), summed[:, 256:512], summed[:, 0:256]
    )
    cos_p, sin_p = cos_sin(place_ref[:, 0:1] * freq_x + place_ref[:, 1:2] * freq_y)

    def along(cos_rows, sin_rows):
        return sin_p * (cos_rows[:, :128] - sin_rows[:, 128:]) + cos_p * (
            sin_rows[:, :128] + cos_rows[:, 128:]
        )

    flat = along(summed[0:ATOMS], summed[ATOMS : 2 * ATOMS])
    force_ref[0] = flat * (TWO_PI / N * freq_x)
    force_ref[1] = flat * (TWO_PI / N * freq_y)
    force_ref[2] = along(summed[2 * ATOMS : 3 * ATOMS], summed[3 * ATOMS : 4 * ATOMS])


def force_kernel(
    psi_ref, miller_ref, radial_ref, place_ref, kind_ref, full_ref, couple_ref, occupy_ref, local_ref, out_ref, mixed_ref
):
    step = pl.program_id(0)

    @pl.when(step == 0)
    def _():
        full = full_ref[...].reshape(SLOTS, ATOMS, 256)
        scale = 2.0 * occupy_ref[...]
        first = []
        second = []
        for j in range(SLOTS):
            mix = couple_ref[:, j : j + 1] * full[0]
            for i in range(1, SLOTS):
                at = i * SLOTS + j
                mix = mix + couple_ref[:, at : at + 1] * full[i]
            real = mix[:, :128] * scale
            imag = mix[:, 128:] * scale
            first.append(jnp.concatenate([-imag, real], axis=1).astype(BF16))
            second.append(jnp.concatenate([real, imag], axis=1).astype(BF16))
        mixed_ref[...] = jnp.concatenate(first + second, axis=0)
        out_ref[...] = local_ref[...]

    product = lax.dot_general(
        mixed_ref[...], psi_ref[...], (((1,), (1,)), ((), ())), preferred_element_type=F32
    )
    miller = miller_ref[...].astype(F32)
    cos, sin = cos_sin(wave_turns(place_ref, miller))
    kind = kind_ref[:, 0:1] == 1
    with_cos = None
    for slot in range(SLOTS):
        radial = picked_radial(radial_ref, slot, kind)
        at = slot * ATOMS
        one = radial * product[at : at + ATOMS]
        two = radial * product[ATOMS * SLOTS + at : ATOMS * SLOTS + at + ATOMS]
        with_cos, with_sin = (one, two) if with_cos is None else (with_cos + one, with_sin + two)
    value = cos * with_cos + sin * with_sin
    wave = (TWO_PI / N) * miller
    for c in range(3):
        term = value * wave[c : c + 1]
        total = term[:, 0:128]
        for k in range(1, STEP // 128):
            total = total + term[:, 128 * k : 128 * (k + 1)]
        out_ref[c] += total


def whole(shape):
    return pl.BlockSpec(shape, lambda *_: (0,) * len(shape))


def assemble_kernel(*refs):
    turn_ref, out_ref = refs[-2], refs[-1]
    pieces = refs[:-2]
    turn = turn_ref[0]
    core = turn_ref[1]
    for b in range(BAND_COUNT // 2):
        shift = lax.rem(turn - b + 4, 4)
        for c in range(2):
            same = (core == c).astype(jnp.int32)
            index = shift * 2 + 1 - same
            value = pieces[0][...]
            for k in range(1, 8):
                value = jnp.where(index == k, pieces[k][...], value)
            at = PART * (2 * b + c)
            out_ref[:, :, pl.ds(at, PART)] = value[:, :, :PART]


def shards(
    density,
    stick_column,
    vloc,
    positions,
    species,
    psi,
    miller_wave,
    proj_radial,
    proj_count,
    dcoef,
    occupation,
):
    band_index = lax.axis_index(BAND)
    ga_index = lax.axis_index(GA)
    place = jnp.pad(positions.T, ((0, 0), (0, 125)))
    kind = jnp.broadcast_to(species[:, None], (ATOMS, 128))
    columns = stick_column.reshape(GA_COUNT, OWN)
    columns = lax.dynamic_slice_in_dim(columns, band_index * PART, PART, 1)
    own_columns = lax.dynamic_slice_in_dim(columns, ga_index, 1, 0)
    own_columns = jnp.pad(own_columns, ((0, 0), (0, 128 - PART)))
    vloc_here = lax.dynamic_slice_in_dim(vloc, band_index * PART, PART, 2)
    vloc_here = jnp.pad(vloc_here, ((0, 0), (0, 0), (0, 128 - PART)))
    y_table, x_table = plane_tables()

    sticks = pl.pallas_call(
        sticks_kernel,
        out_shape=jax.ShapeDtypeStruct((GA_COUNT, 8, 256), F32),
        scratch_shapes=[
            pltpu.VMEM((2, PLANES * ROWS, 256), BF16),
            pltpu.VMEM((2, 8, STICKS + 128), F32),
        ],
        name="sticks",
    )(
        density,
        columns.reshape(1, STICKS),
        jnp.asarray(fold_table()),
        jnp.asarray(y_table),
        jnp.asarray(x_table),
    )

    steps = WAVES // STEP
    outgoing, waves = pl.pallas_call(
        project_kernel,
        grid=(steps,),
        in_specs=[
            pl.BlockSpec((2 * STEP, 128), lambda g: (g, 0)),
            pl.BlockSpec((3, STEP), lambda g: (0, g)),
            pl.BlockSpec((2, SLOTS, STEP), lambda g: (0, 0, g)),
            whole((ATOMS, 128)),
            whole((ATOMS, 128)),
            whole((256, 256)),
            whole((GA_COUNT, 8, 256)),
        ],
        out_specs=[whole((GA_COUNT, 16, 256)), pl.BlockSpec((STEP, 256), lambda g: (g, 0))],
        out_shape=[
            jax.ShapeDtypeStruct((GA_COUNT, 16, 256), F32),
            jax.ShapeDtypeStruct((WAVES, 256), BF16),
        ],
        scratch_shapes=[pltpu.VMEM((2 * ATOMS * SLOTS, 256), F32)],
        compiler_params=pltpu.CompilerParams(dimension_semantics=("arbitrary",)),
        name="project",
    )(
        psi.reshape(2 * WAVES, 128),
        miller_wave,
        proj_radial,
        place,
        kind,
        jnp.asarray(parts_table()),
        sticks,
    )

    arrived = lax.all_to_all(outgoing, GA, 0, 0, tiled=True)
    summed = arrived[:, 0:8, :].sum(axis=0)
    full = lax.all_to_all(
        jnp.broadcast_to(summed[None], (GA_COUNT, 8, 256)), GA, 0, 0, tiled=True
    )

    own, local = pl.pallas_call(
        depth_kernel,
        grid=(1,),
        in_specs=[
            pl.BlockSpec((GA_COUNT, 8, 256), lambda _: (0, 1, 0)),
            whole((2, 2 * N, 256)),
            whole((2, N, 128)),
            whole((ATOMS, 128)),
            whole((ATOMS, 128)),
            whole((1, 128)),
        ],
        out_specs=[whole((2, N, 128)), whole((3, ATOMS, 128))],
        out_shape=[
            jax.ShapeDtypeStruct((2, N, 128), F32),
            jax.ShapeDtypeStruct((3, ATOMS, 128), F32),
        ],
        name="depth",
    )(arrived, jnp.asarray(depth_tables()), vloc_here, place, kind, own_columns)

    pieces = [own]
    for k in range(1, 4):
        pieces.append(lax.ppermute(own, "band_0", [(i, (i + k) % 4) for i in range(4)]))
    swapped = [lax.ppermute(p, "band_1", [(0, 1), (1, 0)]) for p in pieces]
    ordered = [q for pair in zip(pieces, swapped) for q in pair]
    turns = jnp.stack([lax.axis_index("band_0"), lax.axis_index("band_1")]).astype(jnp.int32)
    density_sticks = pl.pallas_call(
        assemble_kernel,
        in_specs=[pl.BlockSpec(memory_space=pltpu.VMEM)] * 8
        + [pl.BlockSpec(memory_space=pltpu.SMEM)],
        out_shape=jax.ShapeDtypeStruct((2, N, OWN), F32),
        name="assemble",
    )(*ordered, turns)

    live = (jnp.arange(SLOTS, dtype=jnp.int32)[None, :] < proj_count[:, None]).astype(F32)
    table = dcoef * live[:, :, None] * live[:, None, :]
    couple = jnp.where((species == 1)[:, None], table[1].reshape(1, 64), table[0].reshape(1, 64))
    couple = jnp.pad(couple, ((0, 0), (0, 64)))

    force = pl.pallas_call(
        force_kernel,
        grid=(steps,),
        in_specs=[
            pl.BlockSpec((STEP, 256), lambda g: (g, 0)),
            pl.BlockSpec((3, STEP), lambda g: (0, g)),
            pl.BlockSpec((2, SLOTS, STEP), lambda g: (0, 0, g)),
            whole((ATOMS, 128)),
            whole((ATOMS, 128)),
            whole((GA_COUNT, 8, 256)),
            whole((ATOMS, 128)),
            whole((1, 128)),
            whole((3, ATOMS, 128)),
        ],
        out_specs=whole((3, ATOMS, 128)),
        out_shape=jax.ShapeDtypeStruct((3, ATOMS, 128), F32),
        scratch_shapes=[pltpu.VMEM((2 * ATOMS * SLOTS, 256), BF16)],
        compiler_params=pltpu.CompilerParams(dimension_semantics=("arbitrary",)),
        name="force",
    )(
        waves,
        miller_wave,
        proj_radial,
        place,
        kind,
        full,
        couple,
        occupation.reshape(1, 128),
        local,
    )

    flat = jnp.pad(force.sum(axis=2).reshape(1, 1, 3 * ATOMS), ((0, 0), (0, 0), (0, 32)))
    everywhere = lax.all_to_all(
        jnp.broadcast_to(flat, (GA_COUNT * BAND_COUNT, 1, 128)), BAND_GA, 0, 0, tiled=True
    )
    forces = everywhere.sum(axis=0)[0, : 3 * ATOMS].reshape(3, ATOMS)
    return (density_sticks, forces)


def solution(mesh):
    split = Mesh(mesh.devices.reshape(4, 2, 8, 4), ("band_0", "band_1", "ga_0", "ga_1"))
    in_specs = (
        P(GA, None, None),
        P(),
        P(None, None, GA),
        P(),
        P(),
        P(GA, None, BAND),
        P(None, GA),
        P(None, None, GA),
        P(),
        P(),
        P(BAND),
    )
    out_specs = (P(None, None, GA), P())
    return jax.shard_map(
        shards, mesh=split, in_specs=in_specs, out_specs=out_specs, check_vma=False
    )
```

```python
import math

import jax
import jax.numpy as jnp
import numpy as np
from jax import lax
from jax.experimental import pallas as pl
from jax.experimental.pallas import tpu as pltpu
from jax.sharding import Mesh
from jax.sharding import PartitionSpec as P


N = 160
HALF = 81
ATOMS = 32
SLOTS = 8
GA = ("ga_0", "ga_1")
BAND = ("band_0", "band_1")
BAND_GA = ("band_0", "band_1", "ga_0", "ga_1")
GA_COUNT = 32
BAND_COUNT = 8
PLANES = 5
OWN = 640
PART = OWN // BAND_COUNT
STICKS = GA_COUNT * PART
ROWS_E = 88
ROWS_O = 80
ROWS = ROWS_E + ROWS_O
CHUNK = 256
WAVES = 8448
STEP = 768
STEPS = WAVES // STEP
TWO_PI = 2.0 * math.pi
NORM = 1.0 / math.sqrt(N * N * N)
F32 = jnp.float32
BF16 = jnp.bfloat16

COS_POLY = (
    6.528658390045166,
    -25.967599868774414,
    60.16762924194336,
    -85.45014190673828,
    64.93911743164062,
    -19.73920440673828,
    1.0,
)
SIN_POLY = (
    3.2381374835968018,
    -14.899847030639648,
    42.02592849731445,
    -76.70301818847656,
    81.60513305664062,
    -41.34170150756836,
    6.2831854820251465,
)


def split_np(table, pieces):
    out = []
    rest = np.asarray(table, np.float64)
    for _ in range(pieces):
        part = np.asarray(rest, np.float32).astype(BF16)
        out.append(part)
        rest = rest - part.astype(np.float64)
    return out


def angles(a, b):
    return TWO_PI / N * ((np.asarray(a)[:, None] * np.asarray(b)[None, :]) % N)


def fold_table():
    fold = np.zeros((ROWS, N), np.float32)
    for x in range(HALF):
        fold[x, x] = 1.0
        fold[x, (N - x) % N] = 1.0
    for x in range(1, N // 2):
        fold[ROWS_E + x - 1, x] = 1.0
        fold[ROWS_E + x - 1, N - x] = -1.0
    return fold.astype(BF16)


def plane_tables():
    freq = np.arange(HALF)
    cos_y = np.zeros((N, 256))
    sin_y = np.zeros((N, 256))
    for third in range(3):
        cos_y[:, third * HALF : (third + 1) * HALF] = np.cos(angles(np.arange(N), freq))
        sin_y[:, third * HALF : (third + 1) * HALF] = np.sin(angles(np.arange(N), freq))
    cos_hi, cos_lo = split_np(cos_y, 2)
    sin_hi, sin_lo = split_np(sin_y, 2)
    y_table = np.stack([cos_hi, cos_lo, sin_hi, sin_lo])
    cos_x = split_np(np.cos(angles(np.arange(HALF), freq)), 3)
    sin_x = split_np(np.sin(angles(np.arange(1, N // 2), freq)), 3)
    x_table = np.zeros((ROWS, 256), BF16)
    for third in range(3):
        x_table[:HALF, third * HALF : (third + 1) * HALF] = cos_x[third]
        x_table[ROWS_E : ROWS_E + N // 2 - 1, third * HALF : (third + 1) * HALF] = sin_x[third]
    return y_table, x_table


def depth_tables():
    angle = angles(np.arange(N), np.arange(N))
    table = np.zeros((2 * N, GA_COUNT * 8))
    for s in range(GA_COUNT):
        for p in range(PLANES):
            table[:N, 8 * s + p] = np.cos(angle[:, PLANES * s + p])
            table[N:, 8 * s + p] = np.sin(angle[:, PLANES * s + p])
    return np.stack(split_np(table, 2))


def parts_table():
    table = np.zeros((256, 256), np.float32)
    for g in range(128):
        table[g, 2 * g] = 1.0
        table[128 + g, 2 * g + 1] = 1.0
    return table.astype(BF16)


def dot(a, b):
    return jnp.dot(a, b, preferred_element_type=F32)


def halves(value):
    high = value.astype(BF16)
    return high, (value - high.astype(F32)).astype(BF16)


def thirds(value):
    high = value.astype(BF16)
    rest = value - high.astype(F32)
    mid = rest.astype(BF16)
    return high, mid, (rest - mid.astype(F32)).astype(BF16)


def dot_fine(a, b):
    a_high, a_low = halves(a)
    b_high, b_low = halves(b)
    return dot(a_high, b_high) + dot(a_high, b_low) + dot(a_low, b_high)


def cos_sin(turns):
    t = turns - jnp.round(turns)
    s = t * t
    cos = jnp.full_like(s, COS_POLY[0])
    for c in COS_POLY[1:]:
        cos = cos * s + c
    sin = jnp.full_like(s, SIN_POLY[0])
    for c in SIN_POLY[1:]:
        sin = sin * s + c
    return cos, sin * t


def frequency(index):
    return jnp.where(index >= N // 2, index - N, index)


def sticks_kernel(
    band_ref,
    density_ref,
    column_ref,
    fold_ref,
    y_ref,
    x_ref,
    out_ref,
    picked_ref,
    left_ref,
    sums_ref,
    row_ref,
):
    start = PART * band_ref[0]
    tile = start // 128
    near = column_ref[pl.ds(tile, GA_COUNT, stride=PLANES), :]
    far = column_ref[pl.ds(jnp.minimum(tile + 1, PLANES - 1), GA_COUNT, stride=PLANES), :]
    picked = pltpu.roll(jnp.concatenate([near, far], axis=1), 256 - (start - 128 * tile), 1)
    picked = picked[:, :128]
    picked_ref[...] = picked
    for d in range(GA_COUNT):
        row_ref[0:1, pl.ds(PART * d, PART)] = picked[d : d + 1, :PART]
    fold = fold_ref[...]
    folded = []
    for p in range(PLANES):
        high, mid, low = thirds(density_ref[p])
        folded.append(dot(fold, high) + dot(fold, mid) + dot(fold, low))
    folded = jnp.concatenate(folded, axis=0)
    e_high, e_low = halves(folded)
    lane = lax.broadcasted_iota(jnp.int32, (PLANES * ROWS, 256), 1)
    for part in range(2):
        spec = (
            dot(e_high, y_ref[2 * part])
            + dot(e_high, y_ref[2 * part + 1])
            + dot(e_low, y_ref[2 * part])
        )
        high = spec.astype(BF16).astype(F32)
        rest = spec - high
        mid = rest.astype(BF16).astype(F32)
        left = jnp.where(lane < HALF, high, jnp.where(lane < 2 * HALF, mid, rest - mid))
        left_ref[part] = left.astype(BF16)
    row = lax.broadcasted_iota(jnp.int32, (256, CHUNK), 0)
    row = jnp.where(
        row < HALF,
        row,
        jnp.where(row < 2 * HALF, row - HALF, jnp.where(row < 3 * HALF, row - 2 * HALF, -1)),
    )
    for chunk in range(STICKS // CHUNK):
        lanes = pl.ds(chunk * CHUNK, CHUNK)
        column = row_ref[0:1, lanes]
        column_x = lax.div(column, N)
        freq_x = frequency(column_x)
        freq_y = frequency(column - N * column_x)
        hit_x = row == jnp.abs(freq_x)
        hit_y = row == jnp.abs(freq_y)
        sign_x = jnp.where(freq_x < 0, -1.0, 1.0)
        sign_y = jnp.where(freq_y < 0, -1.0, 1.0)
        pick_cx = jnp.where(hit_x, 1.0, 0.0).astype(BF16)
        pick_sx = jnp.where(hit_x, sign_x, 0.0).astype(BF16)
        pick_cy = jnp.where(hit_y, 1.0, 0.0).astype(BF16)
        pick_sy = jnp.where(hit_y, sign_y, 0.0).astype(BF16)
        cos_x = dot(x_ref[0:ROWS_E], pick_cx)
        sin_x = dot(x_ref[ROWS_E:ROWS], pick_sx)
        t_cos = dot(left_ref[0], pick_cy)
        t_sin = dot(left_ref[1], pick_sy)
        real = []
        imag = []
        for p in range(PLANES):
            at = p * ROWS
            mid = at + ROWS_E
            end = at + ROWS
            re = (t_cos[at:mid] * cos_x).reshape(ROWS_E // 8, 8, CHUNK).sum(0) - (
                t_sin[mid:end] * sin_x
            ).reshape(ROWS_O // 8, 8, CHUNK).sum(0)
            im = (t_sin[at:mid] * cos_x).reshape(ROWS_E // 8, 8, CHUNK).sum(0) + (
                t_cos[mid:end] * sin_x
            ).reshape(ROWS_O // 8, 8, CHUNK).sum(0)
            real.append(re.sum(0, keepdims=True))
            imag.append(-im.sum(0, keepdims=True))
        blank = [jnp.zeros((1, CHUNK), F32)] * (8 - PLANES)
        sums_ref[0, :, lanes] = jnp.concatenate(real + blank, axis=0)
        sums_ref[1, :, lanes] = jnp.concatenate(imag + blank, axis=0)
    sums_ref[0, :, pl.ds(STICKS, 128)] = jnp.zeros((8, 128), F32)
    sums_ref[1, :, pl.ds(STICKS, 128)] = jnp.zeros((8, 128), F32)
    lane = lax.broadcasted_iota(jnp.int32, (8, 128), 1)
    row = lax.broadcasted_iota(jnp.int32, (8, 128), 0)
    for d in range(GA_COUNT):
        first = d * PART // 128 * 128
        shift = d * PART - first
        windows = []
        for part in range(2):
            window = sums_ref[part, :, pl.ds(first, 256)]
            if shift:
                window = pltpu.roll(window, 256 - shift, 1)
            windows.append(window[:, :128])
        real, imag = windows
        packed = jnp.where(lane < PART, real, pltpu.roll(imag, PART, 1))
        for p in range(PLANES):
            at = 32 * (p % 4)
            shift = (at - (128 - PART)) % 128
            moved = jnp.broadcast_to(pltpu.roll(imag, shift, 1)[p : p + 1], (8, 128))
            spot = (row == PLANES + p // 4) & (lane >= at) & (lane < at + 32)
            packed = jnp.where(spot, moved, packed)
        out_ref[d] = packed


def picked_radial(radial_ref, slot, lanes, kind):
    return jnp.where(
        kind, radial_ref[1, slot : slot + 1, lanes], radial_ref[0, slot : slot + 1, lanes]
    )


def wave_turns(place, miller):
    return place[:, 0:1] * miller[0:1] + place[:, 1:2] * miller[1:2] + place[:, 2:3] * miller[2:3]


def atom_columns(position_ref, species_ref):
    row = lax.broadcasted_iota(jnp.int32, (8, ATOMS), 0)
    rows = jnp.zeros((8, ATOMS), F32)
    for c in range(3):
        rows = jnp.where(row == c, position_ref[c : c + 1, :], rows)
    rows = jnp.where(row == 3, species_ref[...].astype(F32), rows)
    same = lax.broadcasted_iota(jnp.int32, (ATOMS, ATOMS), 0) == lax.broadcasted_iota(
        jnp.int32, (ATOMS, ATOMS), 1
    )
    unit = jnp.where(same, 1.0, 0.0).astype(BF16)
    high, mid, low = (
        lax.dot_general(unit, part, (((1,), (1,)), ((), ())), preferred_element_type=F32)
        for part in thirds(rows)
    )
    return high + mid + low


def project_kernel(
    psi_ref,
    miller_ref,
    radial_ref,
    sticks_ref,
    position_ref,
    species_ref,
    parts_ref,
    out_ref,
    waves_ref,
    atoms_ref,
    psi_buf,
    waves_buf,
    table_buf,
    miller_buf,
    radial_buf,
    in_sems,
    out_sems,
    side_sems,
):
    def arriving(k):
        rows = pl.ds(2 * STEP * k, 2 * STEP)
        return pltpu.make_async_copy(psi_ref.at[rows], psi_buf.at[rows], in_sems.at[k])

    def leaving(k):
        rows = pl.ds(STEP * k, STEP)
        return pltpu.make_async_copy(waves_buf.at[rows], waves_ref.at[rows], out_sems.at[k])

    sides = [
        pltpu.make_async_copy(miller_ref, miller_buf, side_sems.at[0]),
        pltpu.make_async_copy(radial_ref, radial_buf, side_sems.at[1]),
    ]
    for side in sides:
        side.start()
    for k in range(STEPS):
        arriving(k).start()
    atoms = atom_columns(position_ref, species_ref)
    atoms_ref[:, 0:8] = atoms
    kind = atoms[:, 3:4] > 0.5
    parts = parts_ref[...]
    out_ref[:, 16:24, :] = sticks_ref[...]
    for side in sides:
        side.wait()

    def chunk(k, carry):
        arriving(k).wait()
        for s in range(STEP // 256):
            top = pl.multiple_of(2 * STEP * k + 512 * s, 512)
            both = jnp.concatenate(
                [psi_buf[pl.ds(top, 256), :], psi_buf[pl.ds(top + 256, 256), :]], axis=1
            )
            turned = dot(parts, both).astype(BF16)
            at = pl.multiple_of(STEP * k + 256 * s, 256)
            waves_buf[pl.ds(at, 128), 0:128] = turned[:128, :128]
            waves_buf[pl.ds(at, 128), 128:256] = turned[128:, :128]
            waves_buf[pl.ds(at + 128, 128), 0:128] = turned[:128, 128:]
            waves_buf[pl.ds(at + 128, 128), 128:256] = turned[128:, 128:]
            lanes = pl.ds(at, 256)
            cos, sin = cos_sin(wave_turns(atoms, miller_buf[:, lanes].astype(F32)))
            for slot in range(SLOTS):
                radial = picked_radial(radial_buf, slot, lanes, kind)
                table_buf[pl.ds(ATOMS * slot, ATOMS), lanes] = (radial * cos).astype(BF16)
                table_buf[pl.ds(ATOMS * (SLOTS + slot), ATOMS), lanes] = (radial * sin).astype(
                    BF16
                )
        leaving(k).start()
        return carry

    lax.fori_loop(0, STEPS, chunk, 0)
    rows = ATOMS * SLOTS
    product = dot(table_buf[...], waves_buf[...])
    real = product[0:rows, 0:128] - product[rows : 2 * rows, 128:256]
    imag = product[0:rows, 128:256] + product[rows : 2 * rows, 0:128]
    out_ref[:, 0:8, :] = real.reshape(GA_COUNT, 8, 128)
    out_ref[:, 8:16, :] = imag.reshape(GA_COUNT, 8, 128)
    for k in range(STEPS):
        leaving(k).wait()


def depth_kernel(
    arrived_ref, table_ref, vloc_ref, atoms_ref, column_ref, own_ref, force_ref
):
    packed = arrived_ref[...]
    lane = lax.broadcasted_iota(jnp.int32, (GA_COUNT, 8, 128), 2)
    row = lax.broadcasted_iota(jnp.int32, (GA_COUNT, 8, 128), 1)
    second = pltpu.roll(packed, 128 - PART, 2)
    for p in range(PLANES):
        from_row = PLANES + p // 4
        moved = pltpu.roll(packed, (128 - PART - 32 * (p % 4)) % 128, 2)
        moved = jnp.broadcast_to(moved[:, from_row : from_row + 1, :], (GA_COUNT, 8, 128))
        second = jnp.where((row == p) & (lane >= 128 - PART), moved, second)
    planes = jnp.concatenate(
        [packed.reshape(GA_COUNT * 8, 128), second.reshape(GA_COUNT * 8, 128)], axis=1
    )
    high, low = halves(planes)
    product = dot(table_ref[0], high) + dot(table_ref[0], low) + dot(table_ref[1], high)
    real = (product[:N, :128] + product[N:, 128:]) * NORM
    imag = (product[:N, 128:] - product[N:, :128]) * NORM
    own_ref[0] = real
    own_ref[1] = imag
    atoms = atoms_ref[:, 0:8]
    kind = atoms[:, 3:4] > 0.5
    column = column_ref[...]
    column_x = lax.div(column, N)
    freq_x = frequency(column_x).astype(F32)
    freq_y = frequency(column - N * column_x).astype(F32)
    freq_z = frequency(lax.broadcasted_iota(jnp.int32, (1, N), 1)).astype(F32)
    cos_z, sin_z = cos_sin(atoms[:, 2:3] * freq_z)
    wave_z = TWO_PI / N * freq_z
    left = jnp.concatenate([cos_z, sin_z, cos_z * wave_z, sin_z * wave_z], axis=0)
    fields = []
    for s in range(2):
        fields.append(vloc_ref[s] * real)
        fields.append(vloc_ref[s] * imag)
    summed = dot_fine(left, jnp.concatenate(fields, axis=1))
    summed = jnp.where(
        jnp.concatenate([kind] * 4, axis=0), summed[:, 256:512], summed[:, 0:256]
    )
    cos_p, sin_p = cos_sin(atoms[:, 0:1] * freq_x + atoms[:, 1:2] * freq_y)

    def along(cos_rows, sin_rows):
        return sin_p * (cos_rows[:, :128] - sin_rows[:, 128:]) + cos_p * (
            sin_rows[:, :128] + cos_rows[:, 128:]
        )

    flat = along(summed[0:ATOMS], summed[ATOMS : 2 * ATOMS])
    force_ref[0] = flat * (TWO_PI / N * freq_x)
    force_ref[1] = flat * (TWO_PI / N * freq_y)
    force_ref[2] = along(summed[2 * ATOMS : 3 * ATOMS], summed[3 * ATOMS : 4 * ATOMS])


def force_kernel(
    waves_ref,
    miller_ref,
    radial_ref,
    atoms_ref,
    full_ref,
    couple_ref,
    occupy_ref,
    local_ref,
    out_ref,
    waves_buf,
    mixed_ref,
    sems,
):
    def arriving(k):
        rows = pl.ds(STEP * k, STEP)
        return pltpu.make_async_copy(waves_ref.at[rows], waves_buf.at[rows], sems.at[k])

    for k in range(STEPS):
        arriving(k).start()
    full = [
        full_ref[:, 8 * part : 8 * part + 8, :].reshape(SLOTS, ATOMS, 128) for part in range(2)
    ]
    scale = 2.0 * occupy_ref[...]
    for j in range(SLOTS):
        real = imag = None
        for i in range(SLOTS):
            at = i * SLOTS + j
            weight = jnp.broadcast_to(couple_ref[:, at : at + 1], (ATOMS, 128))
            real = weight * full[0][i] if i == 0 else real + weight * full[0][i]
            imag = weight * full[1][i] if i == 0 else imag + weight * full[1][i]
        real = real * scale
        imag = imag * scale
        rows = pl.ds(ATOMS * j, ATOMS)
        mixed_ref[rows, :] = jnp.concatenate([-imag, real], axis=1).astype(BF16)
        rows = pl.ds(ATOMS * (SLOTS + j), ATOMS)
        mixed_ref[rows, :] = jnp.concatenate([real, imag], axis=1).astype(BF16)
    atoms = atoms_ref[:, 0:8]
    kind = atoms[:, 3:4] > 0.5

    def chunk(k, totals):
        arriving(k).wait()
        totals = list(totals)
        for s in range(STEP // 256):
            at = pl.multiple_of(STEP * k + 256 * s, 256)
            lanes = pl.ds(at, 256)
            product = lax.dot_general(
                mixed_ref[...],
                waves_buf[lanes, :],
                (((1,), (1,)), ((), ())),
                preferred_element_type=F32,
            )
            miller = miller_ref[:, lanes].astype(F32)
            cos, sin = cos_sin(wave_turns(atoms, miller))
            with_cos = with_sin = None
            for slot in range(SLOTS):
                radial = picked_radial(radial_ref, slot, lanes, kind)
                row = slot * ATOMS
                one = radial * product[row : row + ATOMS]
                row += ATOMS * SLOTS
                two = radial * product[row : row + ATOMS]
                with_cos = one if with_cos is None else with_cos + one
                with_sin = two if with_sin is None else with_sin + two
            value = cos * with_cos + sin * with_sin
            wave = (TWO_PI / N) * miller
            for c in range(3):
                term = value * wave[c : c + 1]
                totals[c] = totals[c] + (term[:, :128] + term[:, 128:])
        return tuple(totals)

    totals = lax.fori_loop(0, STEPS, chunk, tuple(local_ref[c] for c in range(3)))
    ones = jnp.ones((8, 128), BF16)
    high, mid, low = (
        lax.dot_general(ones, part, (((1,), (1,)), ((), ())), preferred_element_type=F32)
        for part in thirds(jnp.concatenate(totals, axis=0))
    )
    row = (high + mid + low)[0:1]
    row = jnp.concatenate([row, jnp.zeros((1, 32), F32)], axis=1)
    out_ref[...] = jnp.broadcast_to(row.reshape(1, 1, 128), (GA_COUNT * BAND_COUNT, 1, 128))


def whole(shape):
    return pl.BlockSpec(shape, lambda *_: (0,) * len(shape))


def assemble_kernel(*refs):
    turn_ref, out_ref = refs[-2], refs[-1]
    pieces = refs[:-2]
    turn = turn_ref[0]
    core = turn_ref[1]
    for b in range(BAND_COUNT // 2):
        shift = lax.rem(turn - b + 4, 4)
        for c in range(2):
            same = (core == c).astype(jnp.int32)
            index = shift * 2 + 1 - same
            value = pieces[0][...]
            for k in range(1, 8):
                value = jnp.where(index == k, pieces[k][...], value)
            at = PART * (2 * b + c)
            out_ref[:, :, pl.ds(at, PART)] = value[:, :, :PART]


def shards(
    density,
    stick_column,
    vloc,
    positions,
    species,
    psi,
    miller_wave,
    proj_radial,
    proj_count,
    dcoef,
    occupation,
):
    band_index = lax.axis_index(BAND)
    ga_index = lax.axis_index(GA)
    in_vmem = pl.BlockSpec(memory_space=pltpu.VMEM)
    in_hbm = pl.BlockSpec(memory_space=pl.ANY)
    y_table, x_table = plane_tables()
    sticks, columns = pl.pallas_call(
        sticks_kernel,
        in_specs=[pl.BlockSpec(memory_space=pltpu.SMEM)] + [in_vmem] * 5,
        out_shape=[
            jax.ShapeDtypeStruct((GA_COUNT, 8, 128), F32),
            jax.ShapeDtypeStruct((GA_COUNT, 128), jnp.int32),
        ],
        scratch_shapes=[
            pltpu.VMEM((2, PLANES * ROWS, 256), BF16),
            pltpu.VMEM((2, 8, STICKS + 128), F32),
            pltpu.VMEM((8, STICKS), jnp.int32),
        ],
        name="sticks",
    )(
        band_index.astype(jnp.int32).reshape(1),
        density,
        stick_column.reshape(GA_COUNT * PLANES, 128),
        jnp.asarray(fold_table()),
        jnp.asarray(y_table),
        jnp.asarray(x_table),
    )

    outgoing, waves, atoms = pl.pallas_call(
        project_kernel,
        in_specs=[in_hbm] * 3 + [in_vmem] * 4,
        out_specs=[in_vmem, in_hbm, in_vmem],
        out_shape=[
            jax.ShapeDtypeStruct((GA_COUNT, 24, 128), F32),
            jax.ShapeDtypeStruct((WAVES, 256), BF16),
            jax.ShapeDtypeStruct((ATOMS, 128), F32),
        ],
        scratch_shapes=[
            pltpu.VMEM((2 * WAVES, 128), BF16),
            pltpu.VMEM((WAVES, 256), BF16),
            pltpu.VMEM((2 * ATOMS * SLOTS, WAVES), BF16),
            pltpu.VMEM((3, WAVES), jnp.int32),
            pltpu.VMEM((2, SLOTS, WAVES), F32),
            pltpu.SemaphoreType.DMA((STEPS,)),
            pltpu.SemaphoreType.DMA((STEPS,)),
            pltpu.SemaphoreType.DMA((2,)),
        ],
        name="project",
    )(
        psi.reshape(2 * WAVES, 128),
        miller_wave,
        proj_radial,
        sticks,
        positions,
        species.reshape(1, ATOMS),
        jnp.asarray(parts_table()),
    )

    arrived = lax.all_to_all(outgoing, GA, 0, 0, tiled=True)
    summed = arrived[:, 0:16, :].sum(axis=0)
    full = lax.all_to_all(
        jnp.broadcast_to(summed[None], (GA_COUNT, 16, 128)), GA, 0, 0, tiled=True
    )

    own_columns = lax.dynamic_slice_in_dim(columns, ga_index, 1, 0)
    vloc_here = lax.dynamic_slice_in_dim(vloc, band_index * PART, PART, 2)
    vloc_here = jnp.pad(vloc_here, ((0, 0), (0, 0), (0, 128 - PART)))
    own, local = pl.pallas_call(
        depth_kernel,
        grid=(1,),
        in_specs=[
            pl.BlockSpec((GA_COUNT, 8, 128), lambda _: (0, 2, 0)),
            whole((2, 2 * N, 256)),
            whole((2, N, 128)),
            whole((ATOMS, 128)),
            whole((1, 128)),
        ],
        out_specs=[whole((2, N, 128)), whole((3, ATOMS, 128))],
        out_shape=[
            jax.ShapeDtypeStruct((2, N, 128), F32),
            jax.ShapeDtypeStruct((3, ATOMS, 128), F32),
        ],
        name="depth",
    )(arrived, jnp.asarray(depth_tables()), vloc_here, atoms, own_columns)

    pieces = [own]
    for k in range(1, 4):
        pieces.append(lax.ppermute(own, "band_0", [(i, (i + k) % 4) for i in range(4)]))
    swapped = [lax.ppermute(p, "band_1", [(0, 1), (1, 0)]) for p in pieces]
    ordered = [q for pair in zip(pieces, swapped) for q in pair]
    turns = jnp.stack([lax.axis_index("band_0"), lax.axis_index("band_1")]).astype(jnp.int32)
    density_sticks = pl.pallas_call(
        assemble_kernel,
        in_specs=[pl.BlockSpec(memory_space=pltpu.VMEM)] * 8
        + [pl.BlockSpec(memory_space=pltpu.SMEM)],
        out_shape=jax.ShapeDtypeStruct((2, N, OWN), F32),
        name="assemble",
    )(*ordered, turns)

    live = (jnp.arange(SLOTS, dtype=jnp.int32)[None, :] < proj_count[:, None]).astype(F32)
    table = dcoef * live[:, :, None] * live[:, None, :]
    couple = jnp.where((species == 1)[:, None], table[1].reshape(1, 64), table[0].reshape(1, 64))
    couple = jnp.pad(couple, ((0, 0), (0, 64)))

    outgoing = pl.pallas_call(
        force_kernel,
        in_specs=[in_hbm] + [in_vmem] * 7,
        out_specs=in_vmem,
        out_shape=jax.ShapeDtypeStruct((GA_COUNT * BAND_COUNT, 1, 128), F32),
        scratch_shapes=[
            pltpu.VMEM((WAVES, 256), BF16),
            pltpu.VMEM((2 * ATOMS * SLOTS, 256), BF16),
            pltpu.SemaphoreType.DMA((STEPS,)),
        ],
        name="force",
    )(
        waves,
        miller_wave,
        proj_radial,
        atoms,
        full,
        couple,
        occupation.reshape(1, 128),
        local,
    )
    everywhere = lax.all_to_all(outgoing, BAND_GA, 0, 0, tiled=True)
    forces = everywhere.sum(axis=0)[0, : 3 * ATOMS].reshape(3, ATOMS)
    return (density_sticks, forces)


def solution(mesh):
    split = Mesh(mesh.devices.reshape(4, 2, 8, 4), ("band_0", "band_1", "ga_0", "ga_1"))
    in_specs = (
        P(GA, None, None),
        P(),
        P(None, None, GA),
        P(),
        P(),
        P(GA, None, BAND),
        P(None, GA),
        P(None, None, GA),
        P(),
        P(),
        P(BAND),
    )
    out_specs = (P(None, None, GA), P())
    return jax.shard_map(
        shards, mesh=split, in_specs=in_specs, out_specs=out_specs, check_vma=False
    )
```

```python
import math

import jax
import jax.numpy as jnp
import numpy as np
from jax import lax
from jax.experimental import pallas as pl
from jax.experimental.pallas import tpu as pltpu
from jax.sharding import Mesh
from jax.sharding import PartitionSpec as P


N = 160
HALF = 81
ATOMS = 32
SLOTS = 8
GA = ("ga_0", "ga_1")
BAND = ("band_0", "band_1")
BAND_GA = ("band_0", "band_1", "ga_0", "ga_1")
GA_COUNT = 32
BAND_COUNT = 8
PLANES = 5
OWN = 640
PART = OWN // BAND_COUNT
STICKS = GA_COUNT * PART
ROWS_E = 88
ROWS_O = 80
ROWS = ROWS_E + ROWS_O
CHUNK = 256
WAVES = 8448
STEP = 2816
STEPS = WAVES // STEP
FORCE_STEP = 768
TWO_PI = 2.0 * math.pi
NORM = 1.0 / math.sqrt(N * N * N)
F32 = jnp.float32
BF16 = jnp.bfloat16

COS_POLY = (
    6.528658390045166,
    -25.967599868774414,
    60.16762924194336,
    -85.45014190673828,
    64.93911743164062,
    -19.73920440673828,
    1.0,
)
SIN_POLY = (
    3.2381374835968018,
    -14.899847030639648,
    42.02592849731445,
    -76.70301818847656,
    81.60513305664062,
    -41.34170150756836,
    6.2831854820251465,
)
ROUNDER = 12582912.0


def split_np(table, pieces):
    out = []
    rest = np.asarray(table, np.float64)
    for _ in range(pieces):
        part = np.asarray(rest, np.float32).astype(BF16)
        out.append(part)
        rest = rest - part.astype(np.float64)
    return out


def angles(a, b):
    return TWO_PI / N * ((np.asarray(a)[:, None] * np.asarray(b)[None, :]) % N)


def fold_table():
    fold = np.zeros((ROWS, N), np.float32)
    for x in range(HALF):
        fold[x, x] = 1.0
        fold[x, (N - x) % N] = 1.0
    for x in range(1, N // 2):
        fold[ROWS_E + x - 1, x] = 1.0
        fold[ROWS_E + x - 1, N - x] = -1.0
    return fold.astype(BF16)


def plane_tables():
    freq = np.arange(HALF)
    cos_y = np.zeros((N, 256))
    sin_y = np.zeros((N, 256))
    for third in range(3):
        cos_y[:, third * HALF : (third + 1) * HALF] = np.cos(angles(np.arange(N), freq))
        sin_y[:, third * HALF : (third + 1) * HALF] = np.sin(angles(np.arange(N), freq))
    cos_hi, cos_lo = split_np(cos_y, 2)
    sin_hi, sin_lo = split_np(sin_y, 2)
    y_table = np.stack([cos_hi, cos_lo, sin_hi, sin_lo])
    cos_x = split_np(np.cos(angles(np.arange(HALF), freq)), 3)
    sin_x = split_np(np.sin(angles(np.arange(1, N // 2), freq)), 3)
    x_table = np.zeros((ROWS, 256), BF16)
    for third in range(3):
        x_table[:HALF, third * HALF : (third + 1) * HALF] = cos_x[third]
        x_table[ROWS_E : ROWS_E + N // 2 - 1, third * HALF : (third + 1) * HALF] = sin_x[third]
    return y_table, x_table


def depth_tables():
    angle = angles(np.arange(N), np.arange(N))
    table = np.zeros((2 * N, GA_COUNT * 8))
    for s in range(GA_COUNT):
        for p in range(PLANES):
            table[:N, 8 * s + p] = np.cos(angle[:, PLANES * s + p])
            table[N:, 8 * s + p] = np.sin(angle[:, PLANES * s + p])
    return np.stack(split_np(table, 2))


def parts_table():
    table = np.zeros((256, 256), np.float32)
    for g in range(128):
        table[g, 2 * g] = 1.0
        table[128 + g, 2 * g + 1] = 1.0
    return table.astype(BF16)


def dot(a, b):
    return jnp.dot(a, b, preferred_element_type=F32)


def halves(value):
    high = value.astype(BF16)
    return high, (value - high.astype(F32)).astype(BF16)


def thirds(value):
    high = value.astype(BF16)
    rest = value - high.astype(F32)
    mid = rest.astype(BF16)
    return high, mid, (rest - mid.astype(F32)).astype(BF16)


def dot_fine(a, b):
    a_high, a_low = halves(a)
    b_high, b_low = halves(b)
    return dot(a_high, b_high) + dot(a_high, b_low) + dot(a_low, b_high)


def cos_sin(turns):
    t = turns - ((turns + ROUNDER) - ROUNDER)
    s = t * t
    cos = s * COS_POLY[0] + COS_POLY[1]
    for c in COS_POLY[2:]:
        cos = cos * s + c
    sin = s * SIN_POLY[0] + SIN_POLY[1]
    for c in SIN_POLY[2:]:
        sin = sin * s + c
    return cos, sin * t


def frequency(index):
    return jnp.where(index >= N // 2, index - N, index)


def fill_sticks(
    band_ref,
    density_ref,
    column_ref,
    fold_ref,
    y_ref,
    x_ref,
    out_ref,
    picked_ref,
    left_ref,
    sums_ref,
    row_ref,
):
    start = PART * band_ref[0]
    tile = start // 128
    near = column_ref[pl.ds(tile, GA_COUNT, stride=PLANES), :]
    far = column_ref[pl.ds(jnp.minimum(tile + 1, PLANES - 1), GA_COUNT, stride=PLANES), :]
    picked = pltpu.roll(jnp.concatenate([near, far], axis=1), 256 - (start - 128 * tile), 1)
    picked = picked[:, :128]
    picked_ref[...] = picked
    for d in range(GA_COUNT):
        row_ref[0:1, pl.ds(PART * d, PART)] = picked[d : d + 1, :PART]
    fold = fold_ref[...]
    folded = []
    for p in range(PLANES):
        high, mid, low = thirds(density_ref[p])
        folded.append(dot(fold, high) + dot(fold, mid) + dot(fold, low))
    folded = jnp.concatenate(folded, axis=0)
    e_high, e_low = halves(folded)
    lane = lax.broadcasted_iota(jnp.int32, (PLANES * ROWS, 256), 1)
    for part in range(2):
        spec = (
            dot(e_high, y_ref[2 * part])
            + dot(e_high, y_ref[2 * part + 1])
            + dot(e_low, y_ref[2 * part])
        )
        high = spec.astype(BF16).astype(F32)
        rest = spec - high
        mid = rest.astype(BF16).astype(F32)
        left = jnp.where(lane < HALF, high, jnp.where(lane < 2 * HALF, mid, rest - mid))
        left_ref[part] = left.astype(BF16)
    row = lax.broadcasted_iota(jnp.int32, (256, CHUNK), 0)
    row = jnp.where(
        row < HALF,
        row,
        jnp.where(row < 2 * HALF, row - HALF, jnp.where(row < 3 * HALF, row - 2 * HALF, -1)),
    )
    for chunk in range(STICKS // CHUNK):
        lanes = pl.ds(chunk * CHUNK, CHUNK)
        column = row_ref[0:1, lanes]
        column_x = lax.div(column, N)
        freq_x = frequency(column_x)
        freq_y = frequency(column - N * column_x)
        hit_x = row == jnp.abs(freq_x)
        hit_y = row == jnp.abs(freq_y)
        sign_x = jnp.where(freq_x < 0, -1.0, 1.0)
        sign_y = jnp.where(freq_y < 0, -1.0, 1.0)
        pick_cx = jnp.where(hit_x, 1.0, 0.0).astype(BF16)
        pick_sx = jnp.where(hit_x, sign_x, 0.0).astype(BF16)
        pick_cy = jnp.where(hit_y, 1.0, 0.0).astype(BF16)
        pick_sy = jnp.where(hit_y, sign_y, 0.0).astype(BF16)
        cos_x = dot(x_ref[0:ROWS_E], pick_cx)
        sin_x = dot(x_ref[ROWS_E:ROWS], pick_sx)
        t_cos = dot(left_ref[0], pick_cy)
        t_sin = dot(left_ref[1], pick_sy)
        real = []
        imag = []
        for p in range(PLANES):
            at = p * ROWS
            mid = at + ROWS_E
            end = at + ROWS
            re = (t_cos[at:mid] * cos_x).reshape(ROWS_E // 8, 8, CHUNK).sum(0) - (
                t_sin[mid:end] * sin_x
            ).reshape(ROWS_O // 8, 8, CHUNK).sum(0)
            im = (t_sin[at:mid] * cos_x).reshape(ROWS_E // 8, 8, CHUNK).sum(0) + (
                t_cos[mid:end] * sin_x
            ).reshape(ROWS_O // 8, 8, CHUNK).sum(0)
            real.append(re.sum(0, keepdims=True))
            imag.append(-im.sum(0, keepdims=True))
        blank = [jnp.zeros((1, CHUNK), F32)] * (8 - PLANES)
        sums_ref[0, :, lanes] = jnp.concatenate(real + blank, axis=0)
        sums_ref[1, :, lanes] = jnp.concatenate(imag + blank, axis=0)
    sums_ref[0, :, pl.ds(STICKS, 128)] = jnp.zeros((8, 128), F32)
    sums_ref[1, :, pl.ds(STICKS, 128)] = jnp.zeros((8, 128), F32)
    lane = lax.broadcasted_iota(jnp.int32, (8, 128), 1)
    row = lax.broadcasted_iota(jnp.int32, (8, 128), 0)
    for d in range(GA_COUNT):
        first = d * PART // 128 * 128
        shift = d * PART - first
        windows = []
        for part in range(2):
            window = sums_ref[part, :, pl.ds(first, 256)]
            if shift:
                window = pltpu.roll(window, 256 - shift, 1)
            windows.append(window[:, :128])
        real, imag = windows
        packed = jnp.where(lane < PART, real, pltpu.roll(imag, PART, 1))
        for p in range(PLANES):
            at = 32 * (p % 4)
            shift = (at - (128 - PART)) % 128
            moved = jnp.broadcast_to(pltpu.roll(imag, shift, 1)[p : p + 1], (8, 128))
            spot = (row == PLANES + p // 4) & (lane >= at) & (lane < at + 32)
            packed = jnp.where(spot, moved, packed)
        out_ref[d, 16:24, :] = packed


def picked_radial(radial_ref, slot, lanes, kind):
    return jnp.where(
        kind, radial_ref[1, slot : slot + 1, lanes], radial_ref[0, slot : slot + 1, lanes]
    )


def wave_turns(place, miller):
    return place[:, 0:1] * miller[0:1] + place[:, 1:2] * miller[1:2] + place[:, 2:3] * miller[2:3]


def atom_columns(position_ref, species_ref):
    row = lax.broadcasted_iota(jnp.int32, (8, ATOMS), 0)
    rows = jnp.zeros((8, ATOMS), F32)
    for c in range(3):
        rows = jnp.where(row == c, position_ref[c : c + 1, :], rows)
    rows = jnp.where(row == 3, species_ref[...].astype(F32), rows)
    same = lax.broadcasted_iota(jnp.int32, (ATOMS, ATOMS), 0) == lax.broadcasted_iota(
        jnp.int32, (ATOMS, ATOMS), 1
    )
    unit = jnp.where(same, 1.0, 0.0).astype(BF16)
    high, mid, low = (
        lax.dot_general(unit, part, (((1,), (1,)), ((), ())), preferred_element_type=F32)
        for part in thirds(rows)
    )
    return high + mid + low


def project_kernel(
    band_ref,
    psi_ref,
    miller_hbm,
    radial_hbm,
    density_ref,
    column_ref,
    fold_ref,
    y_ref,
    x_ref,
    position_ref,
    species_ref,
    parts_ref,
    out_ref,
    waves_ref,
    miller_ref,
    radial_ref,
    atoms_ref,
    picked_ref,
    left_ref,
    sums_ref,
    row_ref,
    psi_buf,
    waves_buf,
    table_buf,
    in_sems,
    out_sems,
    side_sems,
):
    def arriving(k):
        rows = pl.ds(2 * STEP * k, 2 * STEP)
        return pltpu.make_async_copy(psi_ref.at[rows], psi_buf.at[rows], in_sems.at[k])

    def leaving(k):
        rows = pl.ds(STEP * k, STEP)
        return pltpu.make_async_copy(waves_buf.at[rows], waves_ref.at[rows], out_sems.at[k])

    sides = [
        pltpu.make_async_copy(miller_hbm, miller_ref, side_sems.at[0]),
        pltpu.make_async_copy(radial_hbm, radial_ref, side_sems.at[1]),
    ]
    for side in sides:
        side.start()
    for k in range(STEPS):
        arriving(k).start()
    fill_sticks(
        band_ref,
        density_ref,
        column_ref,
        fold_ref,
        y_ref,
        x_ref,
        out_ref,
        picked_ref,
        left_ref,
        sums_ref,
        row_ref,
    )
    atoms = atom_columns(position_ref, species_ref)
    atoms_ref[:, 0:8] = atoms
    kind = atoms[:, 3:4] > 0.5
    parts = parts_ref[...]
    for side in sides:
        side.wait()

    def chunk(k, carry):
        arriving(k).wait()
        for s in range(STEP // 256):
            top = pl.multiple_of(2 * STEP * k + 512 * s, 512)
            both = jnp.concatenate(
                [psi_buf[pl.ds(top, 256), :], psi_buf[pl.ds(top + 256, 256), :]], axis=1
            )
            turned = dot(parts, both).astype(BF16)
            at = pl.multiple_of(STEP * k + 256 * s, 256)
            waves_buf[pl.ds(at, 128), 0:128] = turned[:128, :128]
            waves_buf[pl.ds(at, 128), 128:256] = turned[128:, :128]
            waves_buf[pl.ds(at + 128, 128), 0:128] = turned[:128, 128:]
            waves_buf[pl.ds(at + 128, 128), 128:256] = turned[128:, 128:]
            lanes = pl.ds(at, 256)
            cos, sin = cos_sin(wave_turns(atoms, miller_ref[:, lanes].astype(F32)))
            for slot in range(SLOTS):
                radial = picked_radial(radial_ref, slot, lanes, kind)
                table_buf[pl.ds(ATOMS * slot, ATOMS), lanes] = (radial * cos).astype(BF16)
                table_buf[pl.ds(ATOMS * (SLOTS + slot), ATOMS), lanes] = (radial * sin).astype(
                    BF16
                )
        leaving(k).start()
        return carry

    lax.fori_loop(0, STEPS, chunk, 0)
    rows = ATOMS * SLOTS
    product = dot(table_buf[...], waves_buf[...])
    real = product[0:rows, 0:128] - product[rows : 2 * rows, 128:256]
    imag = product[0:rows, 128:256] + product[rows : 2 * rows, 0:128]
    out_ref[:, 0:8, :] = real.reshape(GA_COUNT, 8, 128)
    out_ref[:, 8:16, :] = imag.reshape(GA_COUNT, 8, 128)
    for k in range(STEPS):
        leaving(k).wait()


def depth_kernel(
    arrived_ref, table_ref, vloc_ref, atoms_ref, column_ref, own_ref, force_ref
):
    packed = arrived_ref[:, 16:24, :]
    lane = lax.broadcasted_iota(jnp.int32, (GA_COUNT, 8, 128), 2)
    row = lax.broadcasted_iota(jnp.int32, (GA_COUNT, 8, 128), 1)
    second = pltpu.roll(packed, 128 - PART, 2)
    for p in range(PLANES):
        from_row = PLANES + p // 4
        moved = pltpu.roll(packed, (128 - PART - 32 * (p % 4)) % 128, 2)
        moved = jnp.broadcast_to(moved[:, from_row : from_row + 1, :], (GA_COUNT, 8, 128))
        second = jnp.where((row == p) & (lane >= 128 - PART), moved, second)
    planes = jnp.concatenate(
        [packed.reshape(GA_COUNT * 8, 128), second.reshape(GA_COUNT * 8, 128)], axis=1
    )
    high, low = halves(planes)
    product = dot(table_ref[0], high) + dot(table_ref[0], low) + dot(table_ref[1], high)
    real = (product[:N, :128] + product[N:, 128:]) * NORM
    imag = (product[:N, 128:] - product[N:, :128]) * NORM
    own_ref[0] = real
    own_ref[1] = imag
    atoms = atoms_ref[:, 0:8]
    kind = atoms[:, 3:4] > 0.5
    column = column_ref[...]
    column_x = lax.div(column, N)
    freq_x = frequency(column_x).astype(F32)
    freq_y = frequency(column - N * column_x).astype(F32)
    freq_z = frequency(lax.broadcasted_iota(jnp.int32, (1, N), 1)).astype(F32)
    cos_z, sin_z = cos_sin(atoms[:, 2:3] * freq_z)
    wave_z = TWO_PI / N * freq_z
    left = jnp.concatenate([cos_z, sin_z, cos_z * wave_z, sin_z * wave_z], axis=0)
    fields = []
    for s in range(2):
        fields.append(vloc_ref[s] * real)
        fields.append(vloc_ref[s] * imag)
    summed = dot_fine(left, jnp.concatenate(fields, axis=1))
    summed = jnp.where(
        jnp.concatenate([kind] * 4, axis=0), summed[:, 256:512], summed[:, 0:256]
    )
    cos_p, sin_p = cos_sin(atoms[:, 0:1] * freq_x + atoms[:, 1:2] * freq_y)

    def along(cos_rows, sin_rows):
        return sin_p * (cos_rows[:, :128] - sin_rows[:, 128:]) + cos_p * (
            sin_rows[:, :128] + cos_rows[:, 128:]
        )

    flat = along(summed[0:ATOMS], summed[ATOMS : 2 * ATOMS])
    force_ref[0] = flat * (TWO_PI / N * freq_x)
    force_ref[1] = flat * (TWO_PI / N * freq_y)
    force_ref[2] = along(summed[2 * ATOMS : 3 * ATOMS], summed[3 * ATOMS : 4 * ATOMS])


def force_kernel(
    waves_ref,
    miller_ref,
    radial_ref,
    atoms_ref,
    full_ref,
    couple_ref,
    occupy_ref,
    local_ref,
    out_ref,
    waves_buf,
    mixed_ref,
    sems,
):
    def arriving(k):
        rows = pl.ds(FORCE_STEP * k, FORCE_STEP)
        return pltpu.make_async_copy(waves_ref.at[rows], waves_buf.at[rows], sems.at[k])

    for k in range(WAVES // FORCE_STEP):
        arriving(k).start()
    full = [
        full_ref[:, 8 * part : 8 * part + 8, :].reshape(SLOTS, ATOMS, 128) for part in range(2)
    ]
    scale = 2.0 * occupy_ref[...]
    for j in range(SLOTS):
        real = imag = None
        for i in range(SLOTS):
            at = i * SLOTS + j
            weight = jnp.broadcast_to(couple_ref[:, at : at + 1], (ATOMS, 128))
            real = weight * full[0][i] if i == 0 else real + weight * full[0][i]
            imag = weight * full[1][i] if i == 0 else imag + weight * full[1][i]
        real = real * scale
        imag = imag * scale
        rows = pl.ds(ATOMS * j, ATOMS)
        mixed_ref[rows, :] = jnp.concatenate([-imag, real], axis=1).astype(BF16)
        rows = pl.ds(ATOMS * (SLOTS + j), ATOMS)
        mixed_ref[rows, :] = jnp.concatenate([real, imag], axis=1).astype(BF16)
    atoms = atoms_ref[:, 0:8]
    kind = atoms[:, 3:4] > 0.5

    def chunk(k, totals):
        arriving(k).wait()
        totals = list(totals)
        for s in range(FORCE_STEP // 256):
            at = pl.multiple_of(FORCE_STEP * k + 256 * s, 256)
            lanes = pl.ds(at, 256)
            product = lax.dot_general(
                mixed_ref[...],
                waves_buf[lanes, :],
                (((1,), (1,)), ((), ())),
                preferred_element_type=F32,
            )
            miller = miller_ref[:, lanes].astype(F32)
            cos, sin = cos_sin(wave_turns(atoms, miller))
            with_cos = with_sin = None
            for slot in range(SLOTS):
                radial = picked_radial(radial_ref, slot, lanes, kind)
                row = slot * ATOMS
                one = radial * product[row : row + ATOMS]
                row += ATOMS * SLOTS
                two = radial * product[row : row + ATOMS]
                with_cos = one if with_cos is None else with_cos + one
                with_sin = two if with_sin is None else with_sin + two
            value = cos * with_cos + sin * with_sin
            wave = (TWO_PI / N) * miller
            for c in range(3):
                term = value * wave[c : c + 1]
                totals[c] = totals[c] + (term[:, :128] + term[:, 128:])
        return tuple(totals)

    totals = lax.fori_loop(0, WAVES // FORCE_STEP, chunk, tuple(local_ref[c] for c in range(3)))
    ones = jnp.ones((8, 128), BF16)
    high, mid, low = (
        lax.dot_general(ones, part, (((1,), (1,)), ((), ())), preferred_element_type=F32)
        for part in thirds(jnp.concatenate(totals, axis=0))
    )
    row = (high + mid + low)[0:1]
    row = jnp.concatenate([row, jnp.zeros((1, 32), F32)], axis=1)
    out_ref[...] = jnp.broadcast_to(row.reshape(1, 1, 128), (GA_COUNT * BAND_COUNT, 1, 128))


def far(value):
    return pltpu.with_memory_space_constraint(value, pltpu.HBM)


def kept(value):
    return pltpu.with_memory_space_constraint(value, pltpu.VMEM)


def assemble_kernel(*refs):
    turn_ref, out_ref = refs[-2], refs[-1]
    pieces = refs[:-2]
    turn = turn_ref[0]
    core = turn_ref[1]
    for b in range(BAND_COUNT // 2):
        shift = lax.rem(turn - b + 4, 4)
        for c in range(2):
            same = (core == c).astype(jnp.int32)
            index = shift * 2 + 1 - same
            value = pieces[0][...]
            for k in range(1, 8):
                value = jnp.where(index == k, pieces[k][...], value)
            at = PART * (2 * b + c)
            out_ref[:, :, pl.ds(at, PART)] = value[:, :, :PART]


def shards(
    density,
    stick_column,
    vloc,
    positions,
    species,
    psi,
    miller_wave,
    proj_radial,
    proj_count,
    dcoef,
    occupation,
):
    band_index = lax.axis_index(BAND)
    ga_index = lax.axis_index(GA)
    in_vmem = pl.BlockSpec(memory_space=pltpu.VMEM)
    in_hbm = pl.BlockSpec(memory_space=pl.ANY)
    y_table, x_table = plane_tables()
    outgoing, waves, miller, radial, atoms, columns = pl.pallas_call(
        project_kernel,
        in_specs=[pl.BlockSpec(memory_space=pltpu.SMEM)] + [in_hbm] * 3 + [in_vmem] * 8,
        out_specs=[in_vmem, in_hbm] + [in_vmem] * 4,
        out_shape=[
            jax.ShapeDtypeStruct((GA_COUNT, 24, 128), F32),
            pltpu.HBM((WAVES, 256), BF16),
            pltpu.VMEM((3, WAVES), jnp.int32),
            pltpu.VMEM((2, SLOTS, WAVES), F32),
            pltpu.VMEM((ATOMS, 128), F32),
            pltpu.VMEM((GA_COUNT, 128), jnp.int32),
        ],
        scratch_shapes=[
            pltpu.VMEM((2, PLANES * ROWS, 256), BF16),
            pltpu.VMEM((2, 8, STICKS + 128), F32),
            pltpu.VMEM((8, STICKS), jnp.int32),
            pltpu.VMEM((2 * WAVES, 128), BF16),
            pltpu.VMEM((WAVES, 256), BF16),
            pltpu.VMEM((2 * ATOMS * SLOTS, WAVES), BF16),
            pltpu.SemaphoreType.DMA((STEPS,)),
            pltpu.SemaphoreType.DMA((STEPS,)),
            pltpu.SemaphoreType.DMA((2,)),
        ],
        compiler_params=pltpu.CompilerParams(vmem_limit_bytes=36 * 2**20),
        name="project",
    )(
        band_index.astype(jnp.int32).reshape(1),
        far(psi.reshape(2 * WAVES, 128)),
        far(miller_wave),
        far(proj_radial),
        far(density),
        far(stick_column.reshape(GA_COUNT * PLANES, 128)),
        far(jnp.asarray(fold_table())),
        far(jnp.asarray(y_table)),
        far(jnp.asarray(x_table)),
        far(positions),
        far(species.reshape(1, ATOMS)),
        far(jnp.asarray(parts_table())),
    )

    arrived = lax.all_to_all(outgoing, GA, 0, 0, tiled=True)
    summed = arrived[:, 0:16, :].sum(axis=0)
    full = lax.all_to_all(
        jnp.broadcast_to(summed[None], (GA_COUNT, 16, 128)), GA, 0, 0, tiled=True
    )

    own_columns = lax.dynamic_slice_in_dim(columns, ga_index, 1, 0)
    vloc_here = lax.dynamic_slice_in_dim(vloc, band_index * PART, PART, 2)
    vloc_here = jnp.pad(vloc_here, ((0, 0), (0, 0), (0, 128 - PART)))
    own, local = pl.pallas_call(
        depth_kernel,
        in_specs=[in_vmem] * 5,
        out_specs=[in_vmem] * 2,
        out_shape=[
            pltpu.VMEM((2, N, 128), F32),
            pltpu.VMEM((3, ATOMS, 128), F32),
        ],
        compiler_params=pltpu.CompilerParams(vmem_limit_bytes=12 * 2**20),
        name="depth",
    )(kept(arrived), jnp.asarray(depth_tables()), vloc_here, kept(atoms), own_columns)

    pieces = [own]
    for k in range(1, 4):
        pieces.append(lax.ppermute(own, "band_0", [(i, (i + k) % 4) for i in range(4)]))
    swapped = [lax.ppermute(p, "band_1", [(0, 1), (1, 0)]) for p in pieces]
    ordered = [q for pair in zip(pieces, swapped) for q in pair]
    turns = jnp.stack([lax.axis_index("band_0"), lax.axis_index("band_1")]).astype(jnp.int32)
    density_sticks = pl.pallas_call(
        assemble_kernel,
        in_specs=[pl.BlockSpec(memory_space=pltpu.VMEM)] * 8
        + [pl.BlockSpec(memory_space=pltpu.SMEM)],
        out_shape=jax.ShapeDtypeStruct((2, N, OWN), F32),
        compiler_params=pltpu.CompilerParams(vmem_limit_bytes=16 * 2**20),
        name="assemble",
    )(*[kept(piece) for piece in ordered], turns)

    live = (jnp.arange(SLOTS, dtype=jnp.int32)[None, :] < proj_count[:, None]).astype(F32)
    table = dcoef * live[:, :, None] * live[:, None, :]
    couple = jnp.where((species == 1)[:, None], table[1].reshape(1, 64), table[0].reshape(1, 64))
    couple = jnp.pad(couple, ((0, 0), (0, 64)))

    outgoing = pl.pallas_call(
        force_kernel,
        in_specs=[in_hbm] + [in_vmem] * 7,
        out_specs=in_vmem,
        out_shape=jax.ShapeDtypeStruct((GA_COUNT * BAND_COUNT, 1, 128), F32),
        scratch_shapes=[
            pltpu.VMEM((WAVES, 256), BF16),
            pltpu.VMEM((2 * ATOMS * SLOTS, 256), BF16),
            pltpu.SemaphoreType.DMA((WAVES // FORCE_STEP,)),
        ],
        compiler_params=pltpu.CompilerParams(vmem_limit_bytes=24 * 2**20),
        name="force",
    )(
        far(waves),
        kept(miller),
        kept(radial),
        kept(atoms),
        kept(full),
        couple,
        occupation.reshape(1, 128),
        kept(local),
    )
    everywhere = lax.all_to_all(outgoing, BAND_GA, 0, 0, tiled=True)
    forces = everywhere.sum(axis=0)[0, : 3 * ATOMS].reshape(3, ATOMS)
    return (density_sticks, forces)


def solution(mesh):
    split = Mesh(mesh.devices.reshape(4, 2, 8, 4), ("band_0", "band_1", "ga_0", "ga_1"))
    in_specs = (
        P(GA, None, None),
        P(),
        P(None, None, GA),
        P(),
        P(),
        P(GA, None, BAND),
        P(None, GA),
        P(None, None, GA),
        P(),
        P(),
        P(BAND),
    )
    out_specs = (P(None, None, GA), P())
    return jax.shard_map(
        shards, mesh=split, in_specs=in_specs, out_specs=out_specs, check_vma=False
    )
```

```python
import math

import jax
import jax.numpy as jnp
import numpy as np
from jax import lax
from jax.experimental import pallas as pl
from jax.experimental.pallas import tpu as pltpu
from jax.sharding import Mesh
from jax.sharding import PartitionSpec as P


N = 160
HALF = 81
ATOMS = 32
SLOTS = 8
GA = ("ga_0", "ga_1")
BAND = ("band_0", "band_1")
BAND_GA = ("band_0", "band_1", "ga_0", "ga_1")
GA_COUNT = 32
BAND_COUNT = 8
PLANES = 5
OWN = 640
PART = OWN // BAND_COUNT
STICKS = GA_COUNT * PART
ROWS_E = 88
ROWS_O = 80
ROWS = ROWS_E + ROWS_O
CHUNK = 256
WAVES = 8448
STEP = 2816
STEPS = WAVES // STEP
FORCE_STEP = 2816
TWO_PI = 2.0 * math.pi
NORM = 1.0 / math.sqrt(N * N * N)
F32 = jnp.float32
BF16 = jnp.bfloat16

COS_POLY = (
    6.528658390045166,
    -25.967599868774414,
    60.16762924194336,
    -85.45014190673828,
    64.93911743164062,
    -19.73920440673828,
    1.0,
)
SIN_POLY = (
    3.2381374835968018,
    -14.899847030639648,
    42.02592849731445,
    -76.70301818847656,
    81.60513305664062,
    -41.34170150756836,
    6.2831854820251465,
)
ROUNDER = 12582912.0


def split_np(table, pieces):
    out = []
    rest = np.asarray(table, np.float64)
    for _ in range(pieces):
        part = np.asarray(rest, np.float32).astype(BF16)
        out.append(part)
        rest = rest - part.astype(np.float64)
    return out


def angles(a, b):
    return TWO_PI / N * ((np.asarray(a)[:, None] * np.asarray(b)[None, :]) % N)


def fold_table():
    fold = np.zeros((ROWS, N), np.float32)
    for x in range(HALF):
        fold[x, x] = 1.0
        fold[x, (N - x) % N] = 1.0
    for x in range(1, N // 2):
        fold[ROWS_E + x - 1, x] = 1.0
        fold[ROWS_E + x - 1, N - x] = -1.0
    return fold.astype(BF16)


def plane_tables():
    freq = np.arange(HALF)
    cos_y = np.zeros((N, 256))
    sin_y = np.zeros((N, 256))
    for third in range(3):
        cos_y[:, third * HALF : (third + 1) * HALF] = np.cos(angles(np.arange(N), freq))
        sin_y[:, third * HALF : (third + 1) * HALF] = np.sin(angles(np.arange(N), freq))
    cos_hi, cos_lo = split_np(cos_y, 2)
    sin_hi, sin_lo = split_np(sin_y, 2)
    y_table = np.stack([cos_hi, cos_lo, sin_hi, sin_lo])
    cos_x = split_np(np.cos(angles(np.arange(HALF), freq)), 3)
    sin_x = split_np(np.sin(angles(np.arange(1, N // 2), freq)), 3)
    x_table = np.zeros((ROWS, 256), BF16)
    for third in range(3):
        x_table[:HALF, third * HALF : (third + 1) * HALF] = cos_x[third]
        x_table[ROWS_E : ROWS_E + N // 2 - 1, third * HALF : (third + 1) * HALF] = sin_x[third]
    return y_table, x_table


def depth_tables():
    angle = angles(np.arange(N), np.arange(N))
    table = np.zeros((2 * N, GA_COUNT * 8))
    for s in range(GA_COUNT):
        for p in range(PLANES):
            table[:N, 8 * s + p] = np.cos(angle[:, PLANES * s + p])
            table[N:, 8 * s + p] = np.sin(angle[:, PLANES * s + p])
    return np.stack(split_np(table, 2))


def parts_table():
    table = np.zeros((256, 256), np.float32)
    for g in range(128):
        table[g, 2 * g] = 1.0
        table[128 + g, 2 * g + 1] = 1.0
    return table.astype(BF16)


def dot(a, b):
    return jnp.dot(a, b, preferred_element_type=F32)


def halves(value):
    high = value.astype(BF16)
    return high, (value - high.astype(F32)).astype(BF16)


def thirds(value):
    high = value.astype(BF16)
    rest = value - high.astype(F32)
    mid = rest.astype(BF16)
    return high, mid, (rest - mid.astype(F32)).astype(BF16)


def dot_fine(a, b):
    a_high, a_low = halves(a)
    b_high, b_low = halves(b)
    return dot(a_high, b_high) + dot(a_high, b_low) + dot(a_low, b_high)


def cos_sin(turns):
    t = turns - ((turns + ROUNDER) - ROUNDER)
    s = t * t
    cos = s * COS_POLY[0] + COS_POLY[1]
    for c in COS_POLY[2:]:
        cos = cos * s + c
    sin = s * SIN_POLY[0] + SIN_POLY[1]
    for c in SIN_POLY[2:]:
        sin = sin * s + c
    return cos, sin * t


def frequency(index):
    return jnp.where(index >= N // 2, index - N, index)


def fill_sticks(
    band_ref,
    density_ref,
    column_ref,
    fold_ref,
    y_ref,
    x_ref,
    out_ref,
    picked_ref,
    left_ref,
    sums_ref,
    row_ref,
):
    start = PART * band_ref[0]
    tile = start // 128
    near = column_ref[pl.ds(tile, GA_COUNT, stride=PLANES), :]
    far = column_ref[pl.ds(jnp.minimum(tile + 1, PLANES - 1), GA_COUNT, stride=PLANES), :]
    picked = pltpu.roll(jnp.concatenate([near, far], axis=1), 256 - (start - 128 * tile), 1)
    picked = picked[:, :128]
    picked_ref[...] = picked
    for d in range(GA_COUNT):
        row_ref[0:1, pl.ds(PART * d, PART)] = picked[d : d + 1, :PART]
    fold = fold_ref[...]
    folded = []
    for p in range(PLANES):
        high, mid, low = thirds(density_ref[p])
        folded.append(dot(fold, high) + dot(fold, mid) + dot(fold, low))
    folded = jnp.concatenate(folded, axis=0)
    e_high, e_low = halves(folded)
    lane = lax.broadcasted_iota(jnp.int32, (PLANES * ROWS, 256), 1)
    for part in range(2):
        spec = (
            dot(e_high, y_ref[2 * part])
            + dot(e_high, y_ref[2 * part + 1])
            + dot(e_low, y_ref[2 * part])
        )
        high = spec.astype(BF16).astype(F32)
        rest = spec - high
        mid = rest.astype(BF16).astype(F32)
        left = jnp.where(lane < HALF, high, jnp.where(lane < 2 * HALF, mid, rest - mid))
        left_ref[part] = left.astype(BF16)
    row = lax.broadcasted_iota(jnp.int32, (256, CHUNK), 0)
    row = jnp.where(
        row < HALF,
        row,
        jnp.where(row < 2 * HALF, row - HALF, jnp.where(row < 3 * HALF, row - 2 * HALF, -1)),
    )
    for chunk in range(STICKS // CHUNK):
        lanes = pl.ds(chunk * CHUNK, CHUNK)
        column = row_ref[0:1, lanes]
        column_x = lax.div(column, N)
        freq_x = frequency(column_x)
        freq_y = frequency(column - N * column_x)
        hit_x = row == jnp.abs(freq_x)
        hit_y = row == jnp.abs(freq_y)
        sign_x = jnp.where(freq_x < 0, -1.0, 1.0)
        sign_y = jnp.where(freq_y < 0, -1.0, 1.0)
        pick_cx = jnp.where(hit_x, 1.0, 0.0).astype(BF16)
        pick_sx = jnp.where(hit_x, sign_x, 0.0).astype(BF16)
        pick_cy = jnp.where(hit_y, 1.0, 0.0).astype(BF16)
        pick_sy = jnp.where(hit_y, sign_y, 0.0).astype(BF16)
        cos_x = dot(x_ref[0:ROWS_E], pick_cx)
        sin_x = dot(x_ref[ROWS_E:ROWS], pick_sx)
        t_cos = dot(left_ref[0], pick_cy)
        t_sin = dot(left_ref[1], pick_sy)
        real = []
        imag = []
        for p in range(PLANES):
            at = p * ROWS
            mid = at + ROWS_E
            end = at + ROWS
            re = (t_cos[at:mid] * cos_x).reshape(ROWS_E // 8, 8, CHUNK).sum(0) - (
                t_sin[mid:end] * sin_x
            ).reshape(ROWS_O // 8, 8, CHUNK).sum(0)
            im = (t_sin[at:mid] * cos_x).reshape(ROWS_E // 8, 8, CHUNK).sum(0) + (
                t_cos[mid:end] * sin_x
            ).reshape(ROWS_O // 8, 8, CHUNK).sum(0)
            real.append(re.sum(0, keepdims=True))
            imag.append(-im.sum(0, keepdims=True))
        blank = [jnp.zeros((1, CHUNK), F32)] * (8 - PLANES)
        sums_ref[0, :, lanes] = jnp.concatenate(real + blank, axis=0)
        sums_ref[1, :, lanes] = jnp.concatenate(imag + blank, axis=0)
    sums_ref[0, :, pl.ds(STICKS, 128)] = jnp.zeros((8, 128), F32)
    sums_ref[1, :, pl.ds(STICKS, 128)] = jnp.zeros((8, 128), F32)
    lane = lax.broadcasted_iota(jnp.int32, (8, 128), 1)
    row = lax.broadcasted_iota(jnp.int32, (8, 128), 0)
    for d in range(GA_COUNT):
        first = d * PART // 128 * 128
        shift = d * PART - first
        windows = []
        for part in range(2):
            window = sums_ref[part, :, pl.ds(first, 256)]
            if shift:
                window = pltpu.roll(window, 256 - shift, 1)
            windows.append(window[:, :128])
        real, imag = windows
        packed = jnp.where(lane < PART, real, pltpu.roll(imag, PART, 1))
        for p in range(PLANES):
            at = 32 * (p % 4)
            shift = (at - (128 - PART)) % 128
            moved = jnp.broadcast_to(pltpu.roll(imag, shift, 1)[p : p + 1], (8, 128))
            spot = (row == PLANES + p // 4) & (lane >= at) & (lane < at + 32)
            packed = jnp.where(spot, moved, packed)
        out_ref[d, 16:24, :] = packed


def picked_radial(radial_ref, slot, lanes, kind):
    return jnp.where(
        kind, radial_ref[1, slot : slot + 1, lanes], radial_ref[0, slot : slot + 1, lanes]
    )


def wave_turns(place, miller):
    return place[:, 0:1] * miller[0:1] + place[:, 1:2] * miller[1:2] + place[:, 2:3] * miller[2:3]


def atom_columns(position_ref, species_ref):
    row = lax.broadcasted_iota(jnp.int32, (8, ATOMS), 0)
    rows = jnp.zeros((8, ATOMS), F32)
    for c in range(3):
        rows = jnp.where(row == c, position_ref[c : c + 1, :], rows)
    rows = jnp.where(row == 3, species_ref[...].astype(F32), rows)
    same = lax.broadcasted_iota(jnp.int32, (ATOMS, ATOMS), 0) == lax.broadcasted_iota(
        jnp.int32, (ATOMS, ATOMS), 1
    )
    unit = jnp.where(same, 1.0, 0.0).astype(BF16)
    high, mid, low = (
        lax.dot_general(unit, part, (((1,), (1,)), ((), ())), preferred_element_type=F32)
        for part in thirds(rows)
    )
    return high + mid + low


def project_kernel(
    band_ref,
    psi_ref,
    miller_hbm,
    radial_hbm,
    density_ref,
    column_ref,
    fold_ref,
    y_ref,
    x_ref,
    position_ref,
    species_ref,
    parts_ref,
    out_ref,
    waves_ref,
    miller_ref,
    radial_ref,
    atoms_ref,
    picked_ref,
    left_ref,
    sums_ref,
    row_ref,
    psi_buf,
    waves_buf,
    table_buf,
    in_sems,
    out_sems,
    side_sems,
):
    def arriving(k):
        rows = pl.ds(2 * STEP * k, 2 * STEP)
        return pltpu.make_async_copy(psi_ref.at[rows], psi_buf.at[rows], in_sems.at[k])

    def leaving(k):
        rows = pl.ds(STEP * k, STEP)
        return pltpu.make_async_copy(waves_buf.at[rows], waves_ref.at[rows], out_sems.at[k])

    sides = [
        pltpu.make_async_copy(miller_hbm, miller_ref, side_sems.at[0]),
        pltpu.make_async_copy(radial_hbm, radial_ref, side_sems.at[1]),
    ]
    for side in sides:
        side.start()
    for k in range(STEPS):
        arriving(k).start()
    fill_sticks(
        band_ref,
        density_ref,
        column_ref,
        fold_ref,
        y_ref,
        x_ref,
        out_ref,
        picked_ref,
        left_ref,
        sums_ref,
        row_ref,
    )
    atoms = atom_columns(position_ref, species_ref)
    atoms_ref[:, 0:8] = atoms
    kind = atoms[:, 3:4] > 0.5
    parts = parts_ref[...]
    for side in sides:
        side.wait()

    def chunk(k, carry):
        arriving(k).wait()
        for s in range(STEP // 256):
            top = pl.multiple_of(2 * STEP * k + 512 * s, 512)
            both = jnp.concatenate(
                [psi_buf[pl.ds(top, 256), :], psi_buf[pl.ds(top + 256, 256), :]], axis=1
            )
            turned = dot(parts, both).astype(BF16)
            at = pl.multiple_of(STEP * k + 256 * s, 256)
            waves_buf[pl.ds(at, 128), 0:128] = turned[:128, :128]
            waves_buf[pl.ds(at, 128), 128:256] = turned[128:, :128]
            waves_buf[pl.ds(at + 128, 128), 0:128] = turned[:128, 128:]
            waves_buf[pl.ds(at + 128, 128), 128:256] = turned[128:, 128:]
            lanes = pl.ds(at, 256)
            cos, sin = cos_sin(wave_turns(atoms, miller_ref[:, lanes].astype(F32)))
            for slot in range(SLOTS):
                radial = picked_radial(radial_ref, slot, lanes, kind)
                table_buf[pl.ds(ATOMS * slot, ATOMS), lanes] = (radial * cos).astype(BF16)
                table_buf[pl.ds(ATOMS * (SLOTS + slot), ATOMS), lanes] = (radial * sin).astype(
                    BF16
                )
        leaving(k).start()
        return carry

    lax.fori_loop(0, STEPS, chunk, 0)
    rows = ATOMS * SLOTS
    product = dot(table_buf[...], waves_buf[...])
    real = product[0:rows, 0:128] - product[rows : 2 * rows, 128:256]
    imag = product[0:rows, 128:256] + product[rows : 2 * rows, 0:128]
    out_ref[:, 0:8, :] = real.reshape(GA_COUNT, 8, 128)
    out_ref[:, 8:16, :] = imag.reshape(GA_COUNT, 8, 128)
    for k in range(STEPS):
        leaving(k).wait()


def depth_kernel(
    arrived_ref, table_ref, vloc_ref, atoms_ref, column_ref, own_ref, force_ref
):
    packed = arrived_ref[:, 16:24, :]
    lane = lax.broadcasted_iota(jnp.int32, (GA_COUNT, 8, 128), 2)
    row = lax.broadcasted_iota(jnp.int32, (GA_COUNT, 8, 128), 1)
    second = pltpu.roll(packed, 128 - PART, 2)
    for p in range(PLANES):
        from_row = PLANES + p // 4
        moved = pltpu.roll(packed, (128 - PART - 32 * (p % 4)) % 128, 2)
        moved = jnp.broadcast_to(moved[:, from_row : from_row + 1, :], (GA_COUNT, 8, 128))
        second = jnp.where((row == p) & (lane >= 128 - PART), moved, second)
    planes = jnp.concatenate(
        [packed.reshape(GA_COUNT * 8, 128), second.reshape(GA_COUNT * 8, 128)], axis=1
    )
    high, low = halves(planes)
    product = dot(table_ref[0], high) + dot(table_ref[0], low) + dot(table_ref[1], high)
    real = (product[:N, :128] + product[N:, 128:]) * NORM
    imag = (product[:N, 128:] - product[N:, :128]) * NORM
    own_ref[0] = real
    own_ref[1] = imag
    atoms = atoms_ref[:, 0:8]
    kind = atoms[:, 3:4] > 0.5
    column = column_ref[...]
    column_x = lax.div(column, N)
    freq_x = frequency(column_x).astype(F32)
    freq_y = frequency(column - N * column_x).astype(F32)
    freq_z = frequency(lax.broadcasted_iota(jnp.int32, (1, N), 1)).astype(F32)
    cos_z, sin_z = cos_sin(atoms[:, 2:3] * freq_z)
    wave_z = TWO_PI / N * freq_z
    left = jnp.concatenate([cos_z, sin_z, cos_z * wave_z, sin_z * wave_z], axis=0)
    fields = []
    for s in range(2):
        fields.append(vloc_ref[s] * real)
        fields.append(vloc_ref[s] * imag)
    summed = dot_fine(left, jnp.concatenate(fields, axis=1))
    summed = jnp.where(
        jnp.concatenate([kind] * 4, axis=0), summed[:, 256:512], summed[:, 0:256]
    )
    cos_p, sin_p = cos_sin(atoms[:, 0:1] * freq_x + atoms[:, 1:2] * freq_y)

    def along(cos_rows, sin_rows):
        return sin_p * (cos_rows[:, :128] - sin_rows[:, 128:]) + cos_p * (
            sin_rows[:, :128] + cos_rows[:, 128:]
        )

    flat = along(summed[0:ATOMS], summed[ATOMS : 2 * ATOMS])
    force_ref[0] = flat * (TWO_PI / N * freq_x)
    force_ref[1] = flat * (TWO_PI / N * freq_y)
    force_ref[2] = along(summed[2 * ATOMS : 3 * ATOMS], summed[3 * ATOMS : 4 * ATOMS])


def spread_kernel(arrived_ref, out_ref):
    total = arrived_ref[0, 0:16, :]
    for d in range(1, GA_COUNT):
        total = total + arrived_ref[d, 0:16, :]
    for d in range(GA_COUNT):
        out_ref[d] = total


def force_kernel(
    waves_ref,
    miller_ref,
    radial_ref,
    atoms_ref,
    full_ref,
    couple_ref,
    occupy_ref,
    local_ref,
    out_ref,
    waves_buf,
    mixed_ref,
    sems,
):
    def arriving(k):
        rows = pl.ds(FORCE_STEP * k, FORCE_STEP)
        return pltpu.make_async_copy(waves_ref.at[rows], waves_buf.at[rows], sems.at[k])

    for k in range(WAVES // FORCE_STEP):
        arriving(k).start()
    full = [
        full_ref[:, 8 * part : 8 * part + 8, :].reshape(SLOTS, ATOMS, 128) for part in range(2)
    ]
    scale = 2.0 * occupy_ref[...]
    for j in range(SLOTS):
        real = imag = None
        for i in range(SLOTS):
            at = i * SLOTS + j
            weight = jnp.broadcast_to(couple_ref[:, at : at + 1], (ATOMS, 128))
            real = weight * full[0][i] if i == 0 else real + weight * full[0][i]
            imag = weight * full[1][i] if i == 0 else imag + weight * full[1][i]
        real = real * scale
        imag = imag * scale
        rows = pl.ds(ATOMS * j, ATOMS)
        mixed_ref[rows, :] = jnp.concatenate([-imag, real], axis=1).astype(BF16)
        rows = pl.ds(ATOMS * (SLOTS + j), ATOMS)
        mixed_ref[rows, :] = jnp.concatenate([real, imag], axis=1).astype(BF16)
    atoms = atoms_ref[:, 0:8]
    kind = atoms[:, 3:4] > 0.5

    def chunk(k, totals):
        arriving(k).wait()
        totals = list(totals)
        for s in range(FORCE_STEP // 256):
            at = pl.multiple_of(FORCE_STEP * k + 256 * s, 256)
            lanes = pl.ds(at, 256)
            product = lax.dot_general(
                mixed_ref[...],
                waves_buf[lanes, :],
                (((1,), (1,)), ((), ())),
                preferred_element_type=F32,
            )
            miller = miller_ref[:, lanes].astype(F32)
            cos, sin = cos_sin(wave_turns(atoms, miller))
            with_cos = with_sin = None
            for slot in range(SLOTS):
                radial = picked_radial(radial_ref, slot, lanes, kind)
                row = slot * ATOMS
                one = radial * product[row : row + ATOMS]
                row += ATOMS * SLOTS
                two = radial * product[row : row + ATOMS]
                with_cos = one if with_cos is None else with_cos + one
                with_sin = two if with_sin is None else with_sin + two
            value = cos * with_cos + sin * with_sin
            wave = (TWO_PI / N) * miller
            for c in range(3):
                term = value * wave[c : c + 1]
                totals[c] = totals[c] + (term[:, :128] + term[:, 128:])
        return tuple(totals)

    totals = lax.fori_loop(0, WAVES // FORCE_STEP, chunk, tuple(local_ref[c] for c in range(3)))
    ones = jnp.ones((8, 128), BF16)
    high, mid, low = (
        lax.dot_general(ones, part, (((1,), (1,)), ((), ())), preferred_element_type=F32)
        for part in thirds(jnp.concatenate(totals, axis=0))
    )
    row = (high + mid + low)[0:1]
    row = jnp.concatenate([row, jnp.zeros((1, 32), F32)], axis=1)
    out_ref[...] = jnp.broadcast_to(row.reshape(1, 1, 128), (GA_COUNT * BAND_COUNT, 1, 128))


def far(value):
    return pltpu.with_memory_space_constraint(value, pltpu.HBM)


def kept(value):
    return pltpu.with_memory_space_constraint(value, pltpu.VMEM)


def assemble_kernel(*refs):
    turn_ref, out_ref = refs[-2], refs[-1]
    pieces = refs[:-2]
    turn = turn_ref[0]
    core = turn_ref[1]
    for b in range(BAND_COUNT // 2):
        shift = lax.rem(turn - b + 4, 4)
        for c in range(2):
            same = (core == c).astype(jnp.int32)
            index = shift * 2 + 1 - same
            value = pieces[0][...]
            for k in range(1, 8):
                value = jnp.where(index == k, pieces[k][...], value)
            at = PART * (2 * b + c)
            out_ref[:, :, pl.ds(at, PART)] = value[:, :, :PART]


def shards(
    density,
    stick_column,
    vloc,
    positions,
    species,
    psi,
    miller_wave,
    proj_radial,
    proj_count,
    dcoef,
    occupation,
):
    band_index = lax.axis_index(BAND)
    ga_index = lax.axis_index(GA)
    in_vmem = pl.BlockSpec(memory_space=pltpu.VMEM)
    in_hbm = pl.BlockSpec(memory_space=pl.ANY)
    y_table, x_table = plane_tables()
    outgoing, waves, miller, radial, atoms, columns = pl.pallas_call(
        project_kernel,
        in_specs=[pl.BlockSpec(memory_space=pltpu.SMEM)] + [in_hbm] * 3 + [in_vmem] * 8,
        out_specs=[in_vmem, in_hbm] + [in_vmem] * 4,
        out_shape=[
            jax.ShapeDtypeStruct((GA_COUNT, 24, 128), F32),
            pltpu.HBM((WAVES, 256), BF16),
            pltpu.VMEM((3, WAVES), jnp.int32),
            pltpu.VMEM((2, SLOTS, WAVES), F32),
            pltpu.VMEM((ATOMS, 128), F32),
            pltpu.VMEM((GA_COUNT, 128), jnp.int32),
        ],
        scratch_shapes=[
            pltpu.VMEM((2, PLANES * ROWS, 256), BF16),
            pltpu.VMEM((2, 8, STICKS + 128), F32),
            pltpu.VMEM((8, STICKS), jnp.int32),
            pltpu.VMEM((2 * WAVES, 128), BF16),
            pltpu.VMEM((WAVES, 256), BF16),
            pltpu.VMEM((2 * ATOMS * SLOTS, WAVES), BF16),
            pltpu.SemaphoreType.DMA((STEPS,)),
            pltpu.SemaphoreType.DMA((STEPS,)),
            pltpu.SemaphoreType.DMA((2,)),
        ],
        compiler_params=pltpu.CompilerParams(vmem_limit_bytes=36 * 2**20),
        name="project",
    )(
        band_index.astype(jnp.int32).reshape(1),
        far(psi.reshape(2 * WAVES, 128)),
        far(miller_wave),
        far(proj_radial),
        far(density),
        far(stick_column.reshape(GA_COUNT * PLANES, 128)),
        far(jnp.asarray(fold_table())),
        far(jnp.asarray(y_table)),
        far(jnp.asarray(x_table)),
        far(positions),
        far(species.reshape(1, ATOMS)),
        far(jnp.asarray(parts_table())),
    )

    arrived = lax.all_to_all(outgoing, GA, 0, 0, tiled=True)
    copies = pl.pallas_call(
        spread_kernel,
        in_specs=[in_vmem],
        out_specs=in_vmem,
        out_shape=jax.ShapeDtypeStruct((GA_COUNT, 16, 128), F32),
        compiler_params=pltpu.CompilerParams(vmem_limit_bytes=4 * 2**20),
        name="spread",
    )(kept(arrived))
    full = lax.all_to_all(copies, GA, 0, 0, tiled=True)

    own_columns = lax.dynamic_slice_in_dim(columns, ga_index, 1, 0)
    vloc_here = lax.dynamic_slice_in_dim(vloc, band_index * PART, PART, 2)
    vloc_here = jnp.pad(vloc_here, ((0, 0), (0, 0), (0, 128 - PART)))
    own, local = pl.pallas_call(
        depth_kernel,
        in_specs=[in_vmem] * 5,
        out_specs=[in_vmem] * 2,
        out_shape=[
            pltpu.VMEM((2, N, 128), F32),
            pltpu.VMEM((3, ATOMS, 128), F32),
        ],
        compiler_params=pltpu.CompilerParams(vmem_limit_bytes=12 * 2**20),
        name="depth",
    )(kept(arrived), jnp.asarray(depth_tables()), vloc_here, kept(atoms), own_columns)

    pieces = [own]
    for k in range(1, 4):
        pieces.append(lax.ppermute(own, "band_0", [(i, (i + k) % 4) for i in range(4)]))
    swapped = [lax.ppermute(p, "band_1", [(0, 1), (1, 0)]) for p in pieces]
    ordered = [q for pair in zip(pieces, swapped) for q in pair]
    turns = jnp.stack([lax.axis_index("band_0"), lax.axis_index("band_1")]).astype(jnp.int32)
    density_sticks = pl.pallas_call(
        assemble_kernel,
        in_specs=[pl.BlockSpec(memory_space=pltpu.VMEM)] * 8
        + [pl.BlockSpec(memory_space=pltpu.SMEM)],
        out_shape=jax.ShapeDtypeStruct((2, N, OWN), F32),
        compiler_params=pltpu.CompilerParams(vmem_limit_bytes=16 * 2**20),
        name="assemble",
    )(*[kept(piece) for piece in ordered], turns)

    live = (jnp.arange(SLOTS, dtype=jnp.int32)[None, :] < proj_count[:, None]).astype(F32)
    table = dcoef * live[:, :, None] * live[:, None, :]
    couple = jnp.where((species == 1)[:, None], table[1].reshape(1, 64), table[0].reshape(1, 64))
    couple = jnp.pad(couple, ((0, 0), (0, 64)))

    outgoing = pl.pallas_call(
        force_kernel,
        in_specs=[in_hbm] + [in_vmem] * 7,
        out_specs=in_vmem,
        out_shape=jax.ShapeDtypeStruct((GA_COUNT * BAND_COUNT, 1, 128), F32),
        scratch_shapes=[
            pltpu.VMEM((WAVES, 256), BF16),
            pltpu.VMEM((2 * ATOMS * SLOTS, 256), BF16),
            pltpu.SemaphoreType.DMA((WAVES // FORCE_STEP,)),
        ],
        compiler_params=pltpu.CompilerParams(vmem_limit_bytes=24 * 2**20),
        name="force",
    )(
        far(waves),
        kept(miller),
        kept(radial),
        kept(atoms),
        kept(full),
        couple,
        occupation.reshape(1, 128),
        kept(local),
    )
    everywhere = lax.all_to_all(outgoing, BAND_GA, 0, 0, tiled=True)
    forces = everywhere.sum(axis=0)[0, : 3 * ATOMS].reshape(3, ATOMS)
    return (density_sticks, forces)


def solution(mesh):
    split = Mesh(mesh.devices.reshape(4, 2, 8, 4), ("band_0", "band_1", "ga_0", "ga_1"))
    in_specs = (
        P(GA, None, None),
        P(),
        P(None, None, GA),
        P(),
        P(),
        P(GA, None, BAND),
        P(None, GA),
        P(None, None, GA),
        P(),
        P(),
        P(BAND),
    )
    out_specs = (P(None, None, GA), P())
    return jax.shard_map(
        shards, mesh=split, in_specs=in_specs, out_specs=out_specs, check_vma=False
    )
```

```python
import math

import jax
import jax.numpy as jnp
import numpy as np
from jax import lax
from jax.experimental import pallas as pl
from jax.experimental.pallas import tpu as pltpu
from jax.sharding import Mesh
from jax.sharding import PartitionSpec as P


N = 160
HALF = 81
ATOMS = 32
SLOTS = 8
GA = ("ga_0", "ga_1")
BAND = ("band_0", "band_1")
BAND_GA = ("band_0", "band_1", "ga_0", "ga_1")
GA_COUNT = 32
BAND_COUNT = 8
PLANES = 5
OWN = 640
PART = OWN // BAND_COUNT
STICKS = GA_COUNT * PART
ROWS_E = 88
ROWS_O = 80
ROWS = ROWS_E + ROWS_O
CHUNK = 256
WAVES = 8448
STEP = 2816
STEPS = WAVES // STEP
FORCE_STEP = 2816
TWO_PI = 2.0 * math.pi
NORM = 1.0 / math.sqrt(N * N * N)
F32 = jnp.float32
BF16 = jnp.bfloat16

COS_POLY = (
    6.528658390045166,
    -25.967599868774414,
    60.16762924194336,
    -85.45014190673828,
    64.93911743164062,
    -19.73920440673828,
    1.0,
)
SIN_POLY = (
    3.2381374835968018,
    -14.899847030639648,
    42.02592849731445,
    -76.70301818847656,
    81.60513305664062,
    -41.34170150756836,
    6.2831854820251465,
)
ROUNDER = 12582912.0


def split_np(table, pieces):
    out = []
    rest = np.asarray(table, np.float64)
    for _ in range(pieces):
        part = np.asarray(rest, np.float32).astype(BF16)
        out.append(part)
        rest = rest - part.astype(np.float64)
    return out


def angles(a, b):
    return TWO_PI / N * ((np.asarray(a)[:, None] * np.asarray(b)[None, :]) % N)


def fold_table():
    fold = np.zeros((ROWS, N), np.float32)
    for x in range(HALF):
        fold[x, x] = 1.0
        fold[x, (N - x) % N] = 1.0
    for x in range(1, N // 2):
        fold[ROWS_E + x - 1, x] = 1.0
        fold[ROWS_E + x - 1, N - x] = -1.0
    return fold.astype(BF16)


def plane_tables():
    freq = np.arange(HALF)
    cos_y = np.zeros((N, 256))
    sin_y = np.zeros((N, 256))
    for third in range(3):
        cos_y[:, third * HALF : (third + 1) * HALF] = np.cos(angles(np.arange(N), freq))
        sin_y[:, third * HALF : (third + 1) * HALF] = np.sin(angles(np.arange(N), freq))
    cos_hi, cos_lo = split_np(cos_y, 2)
    sin_hi, sin_lo = split_np(sin_y, 2)
    y_table = np.stack([cos_hi, cos_lo, sin_hi, sin_lo])
    cos_x = split_np(np.cos(angles(np.arange(HALF), freq)), 3)
    sin_x = split_np(np.sin(angles(np.arange(1, N // 2), freq)), 3)
    x_table = np.zeros((ROWS, 256), BF16)
    for third in range(3):
        x_table[:HALF, third * HALF : (third + 1) * HALF] = cos_x[third]
        x_table[ROWS_E : ROWS_E + N // 2 - 1, third * HALF : (third + 1) * HALF] = sin_x[third]
    return y_table, x_table


def depth_tables():
    angle = angles(np.arange(N), np.arange(N))
    table = np.zeros((2 * N, GA_COUNT * 8))
    for s in range(GA_COUNT):
        for p in range(PLANES):
            table[:N, 8 * s + p] = np.cos(angle[:, PLANES * s + p])
            table[N:, 8 * s + p] = np.sin(angle[:, PLANES * s + p])
    return np.stack(split_np(table, 2))


def parts_table():
    table = np.zeros((256, 256), np.float32)
    for g in range(128):
        table[g, 2 * g] = 1.0
        table[128 + g, 2 * g + 1] = 1.0
    return table.astype(BF16)


def dot(a, b):
    return jnp.dot(a, b, preferred_element_type=F32)


def halves(value):
    high = value.astype(BF16)
    return high, (value - high.astype(F32)).astype(BF16)


def thirds(value):
    high = value.astype(BF16)
    rest = value - high.astype(F32)
    mid = rest.astype(BF16)
    return high, mid, (rest - mid.astype(F32)).astype(BF16)


def dot_fine(a, b):
    a_high, a_low = halves(a)
    b_high, b_low = halves(b)
    return dot(a_high, b_high) + dot(a_high, b_low) + dot(a_low, b_high)


def cos_sin(turns):
    t = turns - ((turns + ROUNDER) - ROUNDER)
    s = t * t
    cos = s * COS_POLY[0] + COS_POLY[1]
    for c in COS_POLY[2:]:
        cos = cos * s + c
    sin = s * SIN_POLY[0] + SIN_POLY[1]
    for c in SIN_POLY[2:]:
        sin = sin * s + c
    return cos, sin * t


def frequency(index):
    return jnp.where(index >= N // 2, index - N, index)


def fill_sticks(
    band_ref,
    density_ref,
    column_ref,
    fold_ref,
    y_ref,
    x_ref,
    out_ref,
    picked_ref,
    left_ref,
    sums_ref,
    row_ref,
):
    start = PART * band_ref[0]
    tile = start // 128
    near = column_ref[pl.ds(tile, GA_COUNT, stride=PLANES), :]
    far = column_ref[pl.ds(jnp.minimum(tile + 1, PLANES - 1), GA_COUNT, stride=PLANES), :]
    picked = pltpu.roll(jnp.concatenate([near, far], axis=1), 256 - (start - 128 * tile), 1)
    picked = picked[:, :128]
    picked_ref[...] = picked
    for d in range(GA_COUNT):
        row_ref[0:1, pl.ds(PART * d, PART)] = picked[d : d + 1, :PART]
    fold = fold_ref[...]
    folded = []
    for p in range(PLANES):
        high, low = halves(density_ref[p])
        folded.append(dot(fold, high) + dot(fold, low))
    folded = jnp.concatenate(folded, axis=0)
    e_high, e_low = halves(folded)
    lane = lax.broadcasted_iota(jnp.int32, (PLANES * ROWS, 256), 1)
    for part in range(2):
        spec = (
            dot(e_high, y_ref[2 * part])
            + dot(e_high, y_ref[2 * part + 1])
            + dot(e_low, y_ref[2 * part])
        )
        high = spec.astype(BF16).astype(F32)
        rest = spec - high
        mid = rest.astype(BF16).astype(F32)
        left = jnp.where(lane < HALF, high, jnp.where(lane < 2 * HALF, mid, rest - mid))
        left_ref[part] = left.astype(BF16)
    row = lax.broadcasted_iota(jnp.int32, (256, CHUNK), 0)
    row = jnp.where(
        row < HALF,
        row,
        jnp.where(row < 2 * HALF, row - HALF, jnp.where(row < 3 * HALF, row - 2 * HALF, -1)),
    )
    for chunk in range(STICKS // CHUNK):
        lanes = pl.ds(chunk * CHUNK, CHUNK)
        column = row_ref[0:1, lanes]
        column_x = lax.div(column, N)
        freq_x = frequency(column_x)
        freq_y = frequency(column - N * column_x)
        hit_x = row == jnp.abs(freq_x)
        hit_y = row == jnp.abs(freq_y)
        sign_x = jnp.where(freq_x < 0, -1.0, 1.0)
        sign_y = jnp.where(freq_y < 0, -1.0, 1.0)
        pick_cx = jnp.where(hit_x, 1.0, 0.0).astype(BF16)
        pick_sx = jnp.where(hit_x, sign_x, 0.0).astype(BF16)
        pick_cy = jnp.where(hit_y, 1.0, 0.0).astype(BF16)
        pick_sy = jnp.where(hit_y, sign_y, 0.0).astype(BF16)
        cos_x = dot(x_ref[0:ROWS_E], pick_cx)
        sin_x = dot(x_ref[ROWS_E:ROWS], pick_sx)
        t_cos = dot(left_ref[0], pick_cy)
        t_sin = dot(left_ref[1], pick_sy)
        real = []
        imag = []
        for p in range(PLANES):
            at = p * ROWS
            mid = at + ROWS_E
            end = at + ROWS
            re = (t_cos[at:mid] * cos_x).reshape(ROWS_E // 8, 8, CHUNK).sum(0) - (
                t_sin[mid:end] * sin_x
            ).reshape(ROWS_O // 8, 8, CHUNK).sum(0)
            im = (t_sin[at:mid] * cos_x).reshape(ROWS_E // 8, 8, CHUNK).sum(0) + (
                t_cos[mid:end] * sin_x
            ).reshape(ROWS_O // 8, 8, CHUNK).sum(0)
            real.append(re.sum(0, keepdims=True))
            imag.append(-im.sum(0, keepdims=True))
        blank = [jnp.zeros((1, CHUNK), F32)] * (8 - PLANES)
        sums_ref[0, :, lanes] = jnp.concatenate(real + blank, axis=0)
        sums_ref[1, :, lanes] = jnp.concatenate(imag + blank, axis=0)
    sums_ref[0, :, pl.ds(STICKS, 128)] = jnp.zeros((8, 128), F32)
    sums_ref[1, :, pl.ds(STICKS, 128)] = jnp.zeros((8, 128), F32)
    lane = lax.broadcasted_iota(jnp.int32, (8, 128), 1)
    row = lax.broadcasted_iota(jnp.int32, (8, 128), 0)
    for d in range(GA_COUNT):
        first = d * PART // 128 * 128
        shift = d * PART - first
        windows = []
        for part in range(2):
            window = sums_ref[part, :, pl.ds(first, 256)]
            if shift:
                window = pltpu.roll(window, 256 - shift, 1)
            windows.append(window[:, :128])
        real, imag = windows
        packed = jnp.where(lane < PART, real, pltpu.roll(imag, PART, 1))
        for p in range(PLANES):
            at = 32 * (p % 4)
            shift = (at - (128 - PART)) % 128
            moved = jnp.broadcast_to(pltpu.roll(imag, shift, 1)[p : p + 1], (8, 128))
            spot = (row == PLANES + p // 4) & (lane >= at) & (lane < at + 32)
            packed = jnp.where(spot, moved, packed)
        out_ref[d, 16:24, :] = packed


def picked_radial(radial_ref, slot, lanes, kind):
    return jnp.where(
        kind, radial_ref[1, slot : slot + 1, lanes], radial_ref[0, slot : slot + 1, lanes]
    )


def wave_turns(place, miller):
    return place[:, 0:1] * miller[0:1] + place[:, 1:2] * miller[1:2] + place[:, 2:3] * miller[2:3]


def atom_columns(position_ref, species_ref):
    row = lax.broadcasted_iota(jnp.int32, (8, ATOMS), 0)
    rows = jnp.zeros((8, ATOMS), F32)
    for c in range(3):
        rows = jnp.where(row == c, position_ref[c : c + 1, :], rows)
    rows = jnp.where(row == 3, species_ref[...].astype(F32), rows)
    same = lax.broadcasted_iota(jnp.int32, (ATOMS, ATOMS), 0) == lax.broadcasted_iota(
        jnp.int32, (ATOMS, ATOMS), 1
    )
    unit = jnp.where(same, 1.0, 0.0).astype(BF16)
    high, mid, low = (
        lax.dot_general(unit, part, (((1,), (1,)), ((), ())), preferred_element_type=F32)
        for part in thirds(rows)
    )
    return high + mid + low


def project_kernel(
    band_ref,
    psi_ref,
    miller_hbm,
    radial_hbm,
    density_ref,
    column_ref,
    fold_ref,
    y_ref,
    x_ref,
    position_ref,
    species_ref,
    parts_ref,
    out_ref,
    waves_ref,
    miller_ref,
    radial_ref,
    atoms_ref,
    picked_ref,
    left_ref,
    sums_ref,
    row_ref,
    psi_buf,
    waves_buf,
    table_buf,
    in_sems,
    out_sems,
    side_sems,
):
    def arriving(k):
        rows = pl.ds(2 * STEP * k, 2 * STEP)
        return pltpu.make_async_copy(psi_ref.at[rows], psi_buf.at[rows], in_sems.at[k])

    def leaving(k):
        rows = pl.ds(STEP * k, STEP)
        return pltpu.make_async_copy(waves_buf.at[rows], waves_ref.at[rows], out_sems.at[k])

    sides = [
        pltpu.make_async_copy(miller_hbm, miller_ref, side_sems.at[0]),
        pltpu.make_async_copy(radial_hbm, radial_ref, side_sems.at[1]),
    ]
    for side in sides:
        side.start()
    for k in range(STEPS):
        arriving(k).start()
    fill_sticks(
        band_ref,
        density_ref,
        column_ref,
        fold_ref,
        y_ref,
        x_ref,
        out_ref,
        picked_ref,
        left_ref,
        sums_ref,
        row_ref,
    )
    atoms = atom_columns(position_ref, species_ref)
    atoms_ref[:, 0:8] = atoms
    kind = atoms[:, 3:4] > 0.5
    parts = parts_ref[...]
    for side in sides:
        side.wait()

    def chunk(k, carry):
        arriving(k).wait()
        for s in range(STEP // 256):
            top = pl.multiple_of(2 * STEP * k + 512 * s, 512)
            both = jnp.concatenate(
                [psi_buf[pl.ds(top, 256), :], psi_buf[pl.ds(top + 256, 256), :]], axis=1
            )
            turned = dot(parts, both).astype(BF16)
            at = pl.multiple_of(STEP * k + 256 * s, 256)
            waves_buf[pl.ds(at, 128), 0:128] = turned[:128, :128]
            waves_buf[pl.ds(at, 128), 128:256] = turned[128:, :128]
            waves_buf[pl.ds(at + 128, 128), 0:128] = turned[:128, 128:]
            waves_buf[pl.ds(at + 128, 128), 128:256] = turned[128:, 128:]
            lanes = pl.ds(at, 256)
            cos, sin = cos_sin(wave_turns(atoms, miller_ref[:, lanes].astype(F32)))
            for slot in range(SLOTS):
                radial = picked_radial(radial_ref, slot, lanes, kind)
                table_buf[pl.ds(ATOMS * slot, ATOMS), lanes] = (radial * cos).astype(BF16)
                table_buf[pl.ds(ATOMS * (SLOTS + slot), ATOMS), lanes] = (radial * sin).astype(
                    BF16
                )
        leaving(k).start()
        return carry

    lax.fori_loop(0, STEPS, chunk, 0)
    rows = ATOMS * SLOTS
    product = dot(table_buf[...], waves_buf[...])
    real = product[0:rows, 0:128] - product[rows : 2 * rows, 128:256]
    imag = product[0:rows, 128:256] + product[rows : 2 * rows, 0:128]
    out_ref[:, 0:8, :] = real.reshape(GA_COUNT, 8, 128)
    out_ref[:, 8:16, :] = imag.reshape(GA_COUNT, 8, 128)
    for k in range(STEPS):
        leaving(k).wait()


def depth_kernel(
    arrived_ref, table_ref, vloc_ref, atoms_ref, column_ref, own_ref, force_ref
):
    packed = arrived_ref[:, 16:24, :]
    lane = lax.broadcasted_iota(jnp.int32, (GA_COUNT, 8, 128), 2)
    row = lax.broadcasted_iota(jnp.int32, (GA_COUNT, 8, 128), 1)
    second = pltpu.roll(packed, 128 - PART, 2)
    for p in range(PLANES):
        from_row = PLANES + p // 4
        moved = pltpu.roll(packed, (128 - PART - 32 * (p % 4)) % 128, 2)
        moved = jnp.broadcast_to(moved[:, from_row : from_row + 1, :], (GA_COUNT, 8, 128))
        second = jnp.where((row == p) & (lane >= 128 - PART), moved, second)
    planes = jnp.concatenate(
        [packed.reshape(GA_COUNT * 8, 128), second.reshape(GA_COUNT * 8, 128)], axis=1
    )
    high, low = halves(planes)
    product = dot(table_ref[0], high) + dot(table_ref[0], low) + dot(table_ref[1], high)
    real = (product[:N, :128] + product[N:, 128:]) * NORM
    imag = (product[:N, 128:] - product[N:, :128]) * NORM
    own_ref[0] = real
    own_ref[1] = imag
    atoms = atoms_ref[:, 0:8]
    kind = atoms[:, 3:4] > 0.5
    column = column_ref[...]
    column_x = lax.div(column, N)
    freq_x = frequency(column_x).astype(F32)
    freq_y = frequency(column - N * column_x).astype(F32)
    freq_z = frequency(lax.broadcasted_iota(jnp.int32, (1, N), 1)).astype(F32)
    cos_z, sin_z = cos_sin(atoms[:, 2:3] * freq_z)
    wave_z = TWO_PI / N * freq_z
    left = jnp.concatenate([cos_z, sin_z, cos_z * wave_z, sin_z * wave_z], axis=0)
    fields = []
    for s in range(2):
        fields.append(vloc_ref[s] * real)
        fields.append(vloc_ref[s] * imag)
    summed = dot_fine(left, jnp.concatenate(fields, axis=1))
    summed = jnp.where(
        jnp.concatenate([kind] * 4, axis=0), summed[:, 256:512], summed[:, 0:256]
    )
    cos_p, sin_p = cos_sin(atoms[:, 0:1] * freq_x + atoms[:, 1:2] * freq_y)

    def along(cos_rows, sin_rows):
        return sin_p * (cos_rows[:, :128] - sin_rows[:, 128:]) + cos_p * (
            sin_rows[:, :128] + cos_rows[:, 128:]
        )

    flat = along(summed[0:ATOMS], summed[ATOMS : 2 * ATOMS])
    force_ref[0] = flat * (TWO_PI / N * freq_x)
    force_ref[1] = flat * (TWO_PI / N * freq_y)
    force_ref[2] = along(summed[2 * ATOMS : 3 * ATOMS], summed[3 * ATOMS : 4 * ATOMS])


def spread_kernel(arrived_ref, out_ref):
    total = arrived_ref[0, 0:16, :]
    for d in range(1, GA_COUNT):
        total = total + arrived_ref[d, 0:16, :]
    for d in range(GA_COUNT):
        out_ref[d] = total


def force_kernel(
    waves_ref,
    miller_ref,
    radial_ref,
    atoms_ref,
    full_ref,
    couple_ref,
    occupy_ref,
    local_ref,
    out_ref,
    waves_buf,
    mixed_ref,
    sems,
):
    def arriving(k):
        rows = pl.ds(FORCE_STEP * k, FORCE_STEP)
        return pltpu.make_async_copy(waves_ref.at[rows], waves_buf.at[rows], sems.at[k])

    for k in range(WAVES // FORCE_STEP):
        arriving(k).start()
    full = [
        full_ref[:, 8 * part : 8 * part + 8, :].reshape(SLOTS, ATOMS, 128) for part in range(2)
    ]
    scale = 2.0 * occupy_ref[...]
    for j in range(SLOTS):
        real = imag = None
        for i in range(SLOTS):
            at = i * SLOTS + j
            weight = jnp.broadcast_to(couple_ref[:, at : at + 1], (ATOMS, 128))
            real = weight * full[0][i] if i == 0 else real + weight * full[0][i]
            imag = weight * full[1][i] if i == 0 else imag + weight * full[1][i]
        real = real * scale
        imag = imag * scale
        rows = pl.ds(ATOMS * j, ATOMS)
        mixed_ref[rows, :] = jnp.concatenate([-imag, real], axis=1).astype(BF16)
        rows = pl.ds(ATOMS * (SLOTS + j), ATOMS)
        mixed_ref[rows, :] = jnp.concatenate([real, imag], axis=1).astype(BF16)
    atoms = atoms_ref[:, 0:8]
    kind = atoms[:, 3:4] > 0.5

    def chunk(k, totals):
        arriving(k).wait()
        totals = list(totals)
        for s in range(FORCE_STEP // 256):
            at = pl.multiple_of(FORCE_STEP * k + 256 * s, 256)
            lanes = pl.ds(at, 256)
            product = lax.dot_general(
                mixed_ref[...],
                waves_buf[lanes, :],
                (((1,), (1,)), ((), ())),
                preferred_element_type=F32,
            )
            miller = miller_ref[:, lanes].astype(F32)
            cos, sin = cos_sin(wave_turns(atoms, miller))
            with_cos = with_sin = None
            for slot in range(SLOTS):
                radial = picked_radial(radial_ref, slot, lanes, kind)
                row = slot * ATOMS
                one = radial * product[row : row + ATOMS]
                row += ATOMS * SLOTS
                two = radial * product[row : row + ATOMS]
                with_cos = one if with_cos is None else with_cos + one
                with_sin = two if with_sin is None else with_sin + two
            value = cos * with_cos + sin * with_sin
            wave = (TWO_PI / N) * miller
            for c in range(3):
                term = value * wave[c : c + 1]
                totals[c] = totals[c] + (term[:, :128] + term[:, 128:])
        return tuple(totals)

    totals = lax.fori_loop(0, WAVES // FORCE_STEP, chunk, tuple(local_ref[c] for c in range(3)))
    ones = jnp.ones((8, 128), BF16)
    high, mid, low = (
        lax.dot_general(ones, part, (((1,), (1,)), ((), ())), preferred_element_type=F32)
        for part in thirds(jnp.concatenate(totals, axis=0))
    )
    row = (high + mid + low)[0:1]
    row = jnp.concatenate([row, jnp.zeros((1, 32), F32)], axis=1)
    out_ref[...] = jnp.broadcast_to(row.reshape(1, 1, 128), (GA_COUNT * BAND_COUNT, 1, 128))


def far(value):
    return pltpu.with_memory_space_constraint(value, pltpu.HBM)


def kept(value):
    return pltpu.with_memory_space_constraint(value, pltpu.VMEM)


def assemble_kernel(*refs):
    turn_ref, out_ref = refs[-2], refs[-1]
    pieces = refs[:-2]
    turn = turn_ref[0]
    core = turn_ref[1]
    for b in range(BAND_COUNT // 2):
        shift = lax.rem(turn - b + 4, 4)
        for c in range(2):
            same = (core == c).astype(jnp.int32)
            index = shift * 2 + 1 - same
            value = pieces[0][...]
            for k in range(1, 8):
                value = jnp.where(index == k, pieces[k][...], value)
            at = PART * (2 * b + c)
            out_ref[:, :, pl.ds(at, PART)] = value[:, :, :PART]


def shards(
    density,
    stick_column,
    vloc,
    positions,
    species,
    psi,
    miller_wave,
    proj_radial,
    proj_count,
    dcoef,
    occupation,
):
    band_index = lax.axis_index(BAND)
    ga_index = lax.axis_index(GA)
    in_vmem = pl.BlockSpec(memory_space=pltpu.VMEM)
    in_hbm = pl.BlockSpec(memory_space=pl.ANY)
    y_table, x_table = plane_tables()
    outgoing, waves, miller, radial, atoms, columns = pl.pallas_call(
        project_kernel,
        in_specs=[pl.BlockSpec(memory_space=pltpu.SMEM)] + [in_hbm] * 3 + [in_vmem] * 8,
        out_specs=[in_vmem, in_hbm] + [in_vmem] * 4,
        out_shape=[
            jax.ShapeDtypeStruct((GA_COUNT, 24, 128), F32),
            pltpu.HBM((WAVES, 256), BF16),
            pltpu.VMEM((3, WAVES), jnp.int32),
            pltpu.VMEM((2, SLOTS, WAVES), F32),
            pltpu.VMEM((ATOMS, 128), F32),
            pltpu.VMEM((GA_COUNT, 128), jnp.int32),
        ],
        scratch_shapes=[
            pltpu.VMEM((2, PLANES * ROWS, 256), BF16),
            pltpu.VMEM((2, 8, STICKS + 128), F32),
            pltpu.VMEM((8, STICKS), jnp.int32),
            pltpu.VMEM((2 * WAVES, 128), BF16),
            pltpu.VMEM((WAVES, 256), BF16),
            pltpu.VMEM((2 * ATOMS * SLOTS, WAVES), BF16),
            pltpu.SemaphoreType.DMA((STEPS,)),
            pltpu.SemaphoreType.DMA((STEPS,)),
            pltpu.SemaphoreType.DMA((2,)),
        ],
        compiler_params=pltpu.CompilerParams(vmem_limit_bytes=36 * 2**20),
        name="project",
    )(
        band_index.astype(jnp.int32).reshape(1),
        far(psi.reshape(2 * WAVES, 128)),
        far(miller_wave),
        far(proj_radial),
        far(density),
        far(stick_column.reshape(GA_COUNT * PLANES, 128)),
        far(jnp.asarray(fold_table())),
        far(jnp.asarray(y_table)),
        far(jnp.asarray(x_table)),
        far(positions),
        far(species.reshape(1, ATOMS)),
        far(jnp.asarray(parts_table())),
    )

    arrived = lax.all_to_all(outgoing, GA, 0, 0, tiled=True)
    copies = pl.pallas_call(
        spread_kernel,
        in_specs=[in_vmem],
        out_specs=in_vmem,
        out_shape=jax.ShapeDtypeStruct((GA_COUNT, 16, 128), F32),
        compiler_params=pltpu.CompilerParams(vmem_limit_bytes=4 * 2**20),
        name="spread",
    )(kept(arrived))
    full = lax.all_to_all(copies, GA, 0, 0, tiled=True)

    own_columns = lax.dynamic_slice_in_dim(columns, ga_index, 1, 0)
    vloc_here = lax.dynamic_slice_in_dim(vloc, band_index * PART, PART, 2)
    vloc_here = jnp.pad(vloc_here, ((0, 0), (0, 0), (0, 128 - PART)))
    own, local = pl.pallas_call(
        depth_kernel,
        in_specs=[in_vmem] * 5,
        out_specs=[in_vmem] * 2,
        out_shape=[
            pltpu.VMEM((2, N, 128), F32),
            pltpu.VMEM((3, ATOMS, 128), F32),
        ],
        compiler_params=pltpu.CompilerParams(vmem_limit_bytes=12 * 2**20),
        name="depth",
    )(kept(arrived), jnp.asarray(depth_tables()), vloc_here, kept(atoms), own_columns)

    pieces = [own]
    for k in range(1, 4):
        pieces.append(lax.ppermute(own, "band_0", [(i, (i + k) % 4) for i in range(4)]))
    swapped = [lax.ppermute(p, "band_1", [(0, 1), (1, 0)]) for p in pieces]
    ordered = [q for pair in zip(pieces, swapped) for q in pair]
    turns = jnp.stack([lax.axis_index("band_0"), lax.axis_index("band_1")]).astype(jnp.int32)
    density_sticks = pl.pallas_call(
        assemble_kernel,
        in_specs=[pl.BlockSpec(memory_space=pltpu.VMEM)] * 8
        + [pl.BlockSpec(memory_space=pltpu.SMEM)],
        out_shape=jax.ShapeDtypeStruct((2, N, OWN), F32),
        compiler_params=pltpu.CompilerParams(vmem_limit_bytes=16 * 2**20),
        name="assemble",
    )(*[kept(piece) for piece in ordered], turns)

    live = (jnp.arange(SLOTS, dtype=jnp.int32)[None, :] < proj_count[:, None]).astype(F32)
    table = dcoef * live[:, :, None] * live[:, None, :]
    couple = jnp.where((species == 1)[:, None], table[1].reshape(1, 64), table[0].reshape(1, 64))
    couple = jnp.pad(couple, ((0, 0), (0, 64)))

    outgoing = pl.pallas_call(
        force_kernel,
        in_specs=[in_hbm] + [in_vmem] * 7,
        out_specs=in_vmem,
        out_shape=jax.ShapeDtypeStruct((GA_COUNT * BAND_COUNT, 1, 128), F32),
        scratch_shapes=[
            pltpu.VMEM((WAVES, 256), BF16),
            pltpu.VMEM((2 * ATOMS * SLOTS, 256), BF16),
            pltpu.SemaphoreType.DMA((WAVES // FORCE_STEP,)),
        ],
        compiler_params=pltpu.CompilerParams(vmem_limit_bytes=24 * 2**20),
        name="force",
    )(
        far(waves),
        kept(miller),
        kept(radial),
        kept(atoms),
        kept(full),
        couple,
        occupation.reshape(1, 128),
        kept(local),
    )
    everywhere = lax.all_to_all(outgoing, BAND_GA, 0, 0, tiled=True)
    forces = everywhere.sum(axis=0)[0, : 3 * ATOMS].reshape(3, ATOMS)
    return (density_sticks, forces)


def solution(mesh):
    split = Mesh(mesh.devices.reshape(4, 2, 8, 4), ("band_0", "band_1", "ga_0", "ga_1"))
    in_specs = (
        P(GA, None, None),
        P(),
        P(None, None, GA),
        P(),
        P(),
        P(GA, None, BAND),
        P(None, GA),
        P(None, None, GA),
        P(),
        P(),
        P(BAND),
    )
    out_specs = (P(None, None, GA), P())
    return jax.shard_map(
        shards, mesh=split, in_specs=in_specs, out_specs=out_specs, check_vma=False
    )
```
